32 devices in a mesh: group: 2 (over y), ctx: 2 (over x), ep: 8 (over z, core).
Axes of the slice: x: 2, y: 2, z: 4, core: 2. Of those that a mesh axis runs over, the one named last changes fastest.
Arguments:
- q_latent: bfloat16 [512, 16384], P(('group', 'ctx'), 'ep'), parts along dimension 0, may hold values from -48 to 48
- q_rope: bfloat16 [512, 2048], P(('group', 'ctx'), 'ep'), parts along dimension 0, may hold values from -6 to 6
- latent_keys: bfloat16 [1024, 256], P('group', 'ctx'), parts along dimension 0, may hold values from -8 to 8
- rope_keys: bfloat16 [128, 256], P('group', 'ctx'), parts along dimension 0, may hold values from -8 to 8
- w_uv: bfloat16 [32, 512, 128], P('ep'), may hold values from -0.25 to 0.25
- moe_tokens: bfloat16 [4096, 7168], P(('group', 'ep'), 'ctx'), parts along dimension 0, may hold values from -6 to 6
- norm_gain: float32 [7168], P('ctx'), may hold values from 0.1 to 1.9
- expert_ids: int32 [4096, 2], P(('group', 'ep')), parts along dimension 0, may hold values from 0 to 3, all different within a row; in each aligned block of 256 rows (0 to 255, 256 to 511, ...) at most 192 rows name the same one
- route_scale: float32 [4096, 2], P(('group', 'ep')), parts along dimension 0, may hold values from 0.5 to 2.5
- w_gate: bfloat16 [8, 7168, 512], P('ep', 'ctx'), may hold values from -0.0625 to 0.0625
- w_up: bfloat16 [8, 7168, 512], P('ep', 'ctx'), may hold values from -0.0625 to 0.0625
- w_down: bfloat16 [8, 512, 7168], P('ep', None, 'ctx'), may hold values from -0.1875 to 0.1875
Outputs:
- attn_out: bfloat16 [512, 4096], P(('group', 'ctx'), 'ep'), parts along dimension 0
- moe_out: bfloat16 [4096, 7168], P(('group', 'ep'), 'ctx'), parts along dimension 0
The draws below stay inside these ranges and needn't reach their ends.
There are 2 independent parts, one for each index of `group`. The reference program is written for one: setup_inputs(seed, part) draws one part's arguments, and reference() takes and returns one part's arrays. A program takes and returns all parts, laid end to end along the dimension named above; an argument that names none is the same for every part. Nothing has to cross between parts.
Inputs may be any that keep to these rules, and one draw needn't show every extreme that they name: `expert_ids`: each row names 2 different experts; among the rows of one ep index no expert is named more than 192 times, a bound that some block reaches.
All inputs are finite; a program needn't handle non-finite values.
Results may differ from the reference program's by a relative error of at most 0.024.
Values may be sent and summed in bfloat16 or wider, within the bound.
A program may use at most 128 MiB of HBM per device.

```python
import math
import jax
import jax.numpy as jnp
import numpy as np
from jax import lax

D = 7168
LATENT = 512
ROPE = 64
VDIM = 128
FF = 1024
TOP = 2
TOK_DEV = 256
SEQ = 256
HEADS = 32
MTOK = 2048
EXP = 4
FH = 512
CAP = 192
N_EP = 8


def attention_draw(base_key):
    key_base = jax.random.fold_in(base_key, 41)
    keys_all = jax.random.split(key_base, 4)
    query_lat = jnp.clip(jax.random.normal(keys_all[0], (SEQ, HEADS, LATENT), jnp.float32), -6.0, 6.0)
    query_rot = jnp.clip(jax.random.normal(keys_all[1], (SEQ, HEADS, ROPE), jnp.float32), -6.0, 6.0)
    key_lat = jnp.clip(jax.random.normal(keys_all[2], (SEQ, LATENT), jnp.float32), -6.0, 6.0)
    key_rot = jnp.clip(jax.random.normal(keys_all[3], (SEQ, ROPE), jnp.float32), -6.0, 6.0)
    return (query_lat.reshape(SEQ, HEADS * LATENT), query_rot.reshape(SEQ, HEADS * ROPE), key_lat.T, key_rot.T)


def draw_q_latent(key, part):
    return attention_draw(key)[0].astype(jnp.bfloat16)


def draw_q_rope(key, part):
    return attention_draw(key)[1].astype(jnp.bfloat16)


def draw_latent_keys(key, part):
    return attention_draw(key)[2].astype(jnp.bfloat16)


def draw_rope_keys(key, part):
    return attention_draw(key)[3].astype(jnp.bfloat16)


def shard_levels(rng, shape, cuts, least, high):
    loudness, own = 1.0, jax.random.fold_in(rng, 6)
    for axis_at, parts in cuts:
        steps = jnp.exp(jax.random.uniform(jax.random.fold_in(own, axis_at), (parts,), jnp.float32, least / len(cuts), high / len(cuts)))
        loudness = loudness * jnp.repeat(steps, shape[axis_at] // parts).reshape([-1 if axis == axis_at else 1 for axis in range(len(shape))])
    return loudness


def deal_out(rng, own, number, rows, amount, top, bound, skew):
    sequence = jax.random.permutation(rng, amount)
    packed, usual = load_shares(amount, rows * top, bound, skew, True), load_shares(amount, rows * top, bound, skew, False)
    places = jnp.arange(amount)

    def named(tallies, turn):
        used = int((tallies > 0).sum())
        fixed = max(1, used // 4)
        moved = fixed + (places - fixed + turn * (used - fixed)) % max(1, amount - fixed)
        return jnp.zeros((amount,), jnp.int32).at[sequence[jnp.where(places < fixed, places, moved)]].set(jnp.asarray(tallies, jnp.int32))

    tallies = jnp.where(number % 4 == 0, named(packed, number // 4), named(usual, number - number // 4 - 1))
    mixed = jax.random.permutation(jax.random.fold_in(own, 3), amount)
    giver, taker = mixed[0:amount // 2 * 2:2], mixed[1:amount // 2 * 2:2]
    slack = jnp.minimum(tallies[giver] - 1, bound - tallies[taker]) // 2
    slack = jnp.where((giver == sequence[0]) | (taker == sequence[0]) | (tallies[taker] == 0), 0, jnp.maximum(slack, 0))
    moved = jax.random.randint(jax.random.fold_in(own, 4), (amount // 2,), 0, 1 << 20) % (slack + 1)
    tallies = tallies.at[giver].add(-moved).at[taker].add(moved)
    members = jnp.searchsorted(jnp.cumsum(tallies), jnp.arange(rows * top), side="right").astype(jnp.int32)
    listing = members.reshape(top, rows).T
    listing = listing[jax.random.permutation(jax.random.fold_in(own, 1), rows)]
    turn = jax.random.randint(jax.random.fold_in(own, 2), (rows, 1), 0, top)
    return jnp.take_along_axis(listing, (jnp.arange(top)[None, :] + turn) % top, axis=1)


def load_shares(number_of, total, limit, lean, full):
    portions = [(1 << 20) // math.isqrt(standing ** lean) + 1 for standing in range(1, number_of + 1)]
    largest = limit if full else min(limit, max(-(-total // number_of), total * portions[0] // sum(portions)))
    least = 1 if total - largest >= number_of - 1 else 0
    given, rest = [largest] + [least] * (number_of - 1), total - largest - least * (number_of - 1)
    while rest > 0:
        movable = [i for i in range(1, number_of) if given[i] < largest] or [i for i in range(1, number_of) if given[i] < limit]
        pool, left = sum([portions[i] for i in movable]), rest
        for i in movable:
            extra = min(limit - given[i], max(1, left * portions[i] // pool), rest)
            given[i] = given[i] + extra
            rest = rest - extra
    return np.array(given)


def bell_draw(rng, shape, scale, most, pieces=(), kind=jnp.bfloat16):
    values = jax.random.normal(rng, shape, jnp.float32) * scale
    if len(pieces) > 0:
        values = shard_levels(rng, shape, pieces, -0.22, 0.18) * values
    return jnp.clip(values, min=-most, max=most).astype(kind)


def setup_inputs(seed: int = 0, part: int = 0) -> dict:
    seeds = jax.random.split(jax.random.key(seed), 13)
    own_keys = jax.random.split(jax.random.fold_in(seeds[12], part), 13)
    q_latent = draw_q_latent(jax.random.fold_in(jax.random.fold_in(seeds[12], part), 71), part)
    q_rope = draw_q_rope(jax.random.fold_in(jax.random.fold_in(seeds[12], part), 71), part)
    latent_keys = draw_latent_keys(jax.random.fold_in(jax.random.fold_in(seeds[12], part), 71), part)
    rope_keys = draw_rope_keys(jax.random.fold_in(jax.random.fold_in(seeds[12], part), 71), part)
    w_uv = bell_draw(seeds[4], (HEADS, LATENT, VDIM), LATENT ** -0.5, 0.25, ((0, 8),))
    moe_tokens = bell_draw(own_keys[5], (MTOK, D), 1.0, 6.0, ((0, 8), (1, 2)))
    norm_gain = jnp.clip(1.0 + 0.18 * jax.random.normal(seeds[6], (D,), jnp.float32), 0.1, 1.9)
    expert_ids_keys = jax.random.split(jax.random.fold_in(own_keys[7], 1), MTOK // TOK_DEV)
    expert_ids_turns = jax.random.permutation(jax.random.fold_in(own_keys[7], 3), MTOK // TOK_DEV)
    expert_ids = jax.vmap(lambda own, number: deal_out(jax.random.fold_in(own_keys[7], 2), own, number, TOK_DEV, EXP, TOP, CAP, 2))(expert_ids_keys, expert_ids_turns).reshape((MTOK, TOP))
    route_scale = jnp.clip(0.5 + 2.0 * jax.random.uniform(own_keys[8], (MTOK, TOP), jnp.float32) ** shard_levels(own_keys[8], (MTOK, TOP), ((0, 8),), -0.2, 0.2), 0.5, 2.5)
    w_gate = bell_draw(seeds[9], (2 * EXP, D, FH), D ** -0.5, 0.0625, ((0, 8), (1, 2)))
    w_up = bell_draw(seeds[10], (2 * EXP, D, FH), D ** -0.5, 0.0625, ((0, 8), (1, 2)))
    w_down = bell_draw(seeds[11], (2 * EXP, FH, D), FF ** -0.5, 0.1875, ((0, 8), (2, 2)))
    return dict(q_latent=q_latent, q_rope=q_rope, latent_keys=latent_keys, rope_keys=rope_keys, w_uv=w_uv, moe_tokens=moe_tokens, norm_gain=norm_gain, expert_ids=expert_ids, route_scale=route_scale, w_gate=w_gate, w_up=w_up, w_down=w_down)


score_scale = 192.0 ** (-0.5)
norm_eps = 1e-06

def reference(q_latent, q_rope, latent_keys, rope_keys, w_uv, moe_tokens, norm_gain, expert_ids, route_scale, w_gate, w_up, w_down):
    positions = jnp.arange(SEQ, dtype=jnp.int32)
    visible = positions[None, :] <= positions[:, None]

    def one_head(head_index):
        query_lat = lax.dynamic_slice_in_dim(q_latent, head_index * LATENT, LATENT, 1)
        query_rot = lax.dynamic_slice_in_dim(q_rope, head_index * ROPE, ROPE, 1)
        scores = jnp.dot(query_lat, latent_keys, preferred_element_type=jnp.float32)
        scores = (scores + jnp.dot(query_rot, rope_keys, preferred_element_type=jnp.float32)) * score_scale
        scores = jnp.where(visible, scores, -jnp.inf)
        row_max = lax.optimization_barrier(jnp.max(scores, axis=1, keepdims=True))
        exponent = jnp.exp(scores - row_max)
        row_total = lax.optimization_barrier(jnp.sum(exponent, axis=1, keepdims=True))
        probabilities = exponent.astype(jnp.bfloat16)
        mixed = jnp.dot(probabilities, latent_keys.T, preferred_element_type=jnp.float32) / row_total
        context = mixed.astype(jnp.bfloat16)
        return jnp.dot(context, w_uv[head_index], preferred_element_type=jnp.float32).astype(jnp.bfloat16)
    heads_out = lax.map(one_head, jnp.arange(HEADS, dtype=jnp.int32))
    attn_out = heads_out.transpose(1, 0, 2).reshape(SEQ, HEADS * VDIM)
    tokens_wide = moe_tokens.astype(jnp.float32)
    mean_square = lax.optimization_barrier(jnp.mean(tokens_wide * tokens_wide, axis=1, keepdims=True))
    normed = (tokens_wide * lax.rsqrt(mean_square + norm_eps) * norm_gain[None, :]).astype(jnp.bfloat16)
    flat_ids = expert_ids.reshape(-1)
    route_token = jnp.arange(MTOK * TOP, dtype=jnp.int32) // TOP
    source = route_token // TOK_DEV
    onehot = (flat_ids[:, None] == jnp.arange(EXP, dtype=jnp.int32)[None, :]).astype(jnp.int32)
    blocked = onehot.reshape(N_EP, TOK_DEV * TOP, EXP)
    slot_index = lax.optimization_barrier(jnp.sum((jnp.cumsum(blocked, axis=1) - blocked) * blocked, axis=2)).reshape(-1)
    row_index = source * CAP + slot_index
    scale_flat = route_scale.reshape(-1)
    total_rows = N_EP * CAP

    def scan_step(running, expert_index):
        chosen = flat_ids == expert_index
        destination = jnp.where(chosen, row_index, total_rows).astype(jnp.int32)
        token_at = jnp.zeros((total_rows,), jnp.int32).at[destination].set(route_token, mode='drop')
        scale_at = jnp.zeros((total_rows,), jnp.float32).at[destination].set(scale_flat, mode='drop')
        rows_taken = normed[token_at]
        output_sum = jnp.zeros((total_rows, D), jnp.float32)
        for half_index in range(2):
            block_index = 2 * expert_index + half_index
            gate_val = jnp.dot(rows_taken, w_gate[block_index], preferred_element_type=jnp.float32)
            up_val = jnp.dot(rows_taken, w_up[block_index], preferred_element_type=jnp.float32)
            hidden = (jax.nn.silu(gate_val) * up_val).astype(jnp.bfloat16)
            piece_out = jnp.dot(hidden, w_down[block_index], preferred_element_type=jnp.float32).astype(jnp.bfloat16)
            piece_out = lax.optimization_barrier(piece_out)
            output_sum = output_sum + piece_out.astype(jnp.float32)
        contribution = output_sum * scale_at[:, None]
        return (running + jax.ops.segment_sum(contribution, token_at, num_segments=MTOK), None)
    moe_sum, ignored = lax.scan(scan_step, jnp.zeros((MTOK, D), jnp.float32), jnp.arange(EXP, dtype=jnp.int32))
    return (attn_out, moe_sum.astype(jnp.bfloat16))
```

```python
import functools
import jax
import jax.numpy as jnp
from jax import lax
from jax.experimental import pallas as pl
from jax.experimental.pallas import tpu as pltpu
from jax.sharding import PartitionSpec as P

score_scale = 192.0 ** (-0.5)
norm_eps = 1e-06
neg_large = -1e30
PIECES = 2
CHUNKS = 4
SLACK = 1
VMEM_BYTES = 67043328
f32 = jnp.float32
bf16 = jnp.bfloat16


def mm(a, b):
    return jnp.dot(a, b, preferred_element_type=f32)


def mm_t(a, b):
    return lax.dot_general(a, b, (((0,), (0,)), ((), ())), preferred_element_type=f32)


def swap_ctx(x):
    return lax.ppermute(x, "ctx", [(0, 1), (1, 0)])


def gather_keys(mine, ctx):
    if lax.axis_size("ctx") != 2:
        return lax.all_gather(mine, "ctx", axis=1, tiled=True)
    other = swap_ctx(mine)
    first = ctx == 0
    return jnp.concatenate(
        [jnp.where(first, mine, other), jnp.where(first, other, mine)], axis=1
    )


def sum_ctx(x):
    if lax.axis_size("ctx") != 2:
        return lax.psum(x, "ctx")
    return x + swap_ctx(x)


def attention(q_latent, q_rope, latent_keys, rope_keys, w_uv):
    seq_rows = q_latent.shape[0]
    head_count = w_uv.shape[0]
    latent_dim = latent_keys.shape[0]
    rope_dim = rope_keys.shape[0]
    query_lat = (
        q_latent.reshape(seq_rows, head_count, latent_dim)
        .transpose(1, 0, 2)
        .reshape(head_count * seq_rows, latent_dim)
    )
    query_rot = (
        q_rope.reshape(seq_rows, head_count, rope_dim)
        .transpose(1, 0, 2)
        .reshape(head_count * seq_rows, rope_dim)
    )
    ctx = lax.axis_index("ctx")
    query_pos = ctx * seq_rows + jnp.tile(jnp.arange(seq_rows, dtype=jnp.int32), head_count)
    mine = jnp.concatenate([latent_keys, rope_keys], axis=0)
    keys = gather_keys(mine, ctx)
    lat, rope = keys[:latent_dim], keys[latent_dim:]
    scores = (mm(query_lat, lat) + mm(query_rot, rope)) * score_scale
    key_pos = jnp.arange(lat.shape[1], dtype=jnp.int32)
    visible = key_pos[None, :] <= query_pos[:, None]
    masked = jnp.where(visible, scores, neg_large)
    top = jnp.max(masked, axis=1, keepdims=True)
    weights = jnp.where(visible, jnp.exp(masked - top), 0.0)
    total = jnp.sum(weights, axis=1, keepdims=True)
    update = lax.dot_general(
        weights.astype(bf16), lat, (((1,), (1,)), ((), ())), preferred_element_type=f32
    )
    context = (update / total).astype(bf16).reshape(head_count, seq_rows, latent_dim)
    heads = jnp.einsum("hsl,hlv->shv", context, w_uv, preferred_element_type=f32)
    return heads.reshape(seq_rows, head_count * w_uv.shape[2]).astype(bf16)


def ranks(key):
    n = key.shape[0]
    at = jnp.arange(n, dtype=jnp.int32)
    ahead = (key[None, :] > key[:, None]) | (
        (key[None, :] == key[:, None]) & (at[None, :] < at[:, None])
    )
    return jnp.sum(ahead.astype(jnp.int32), axis=1)


def position(ids, to_right):
    return ranks(jnp.where(to_right, jnp.max(ids, axis=1), -jnp.min(ids, axis=1)))


def hop_body(
    q_latent,
    q_rope,
    latent_keys,
    rope_keys,
    w_uv,
    moe_tokens,
    norm_gain,
    expert_ids,
    route_scale,
    w_gate,
    w_up,
    w_down,
):
    n_ep = lax.axis_size("ep")
    nz = n_ep // 2
    rows, top_count = expert_ids.shape
    cap = min(rows, 3 * rows * top_count // (2 * nz))
    half = cap // 2
    width = moe_tokens.shape[1]
    ep = lax.axis_index("ep")
    z = ep // 2
    ctx = lax.axis_index("ctx")
    group = -(-128 // cap)
    bands = [
        (b, cap * b, min(rows, cap * (b + group)))
        for b in range(0, nz - 1, group)
        if cap * b < rows
    ]
    pieces = max(1, PIECES * width // 3584)

    def hop(x, pairs):
        return lax.ppermute(
            x, "ep", [(2 * a + c, 2 * b + c) for a, b in pairs for c in range(2)]
        )

    info = jnp.concatenate([expert_ids.astype(f32), route_scale], axis=1)
    infos = {0: info}
    for k in range(1, nz):
        infos[k] = hop(info, [(a, (a + k) % nz) for a in range(nz)])

    def partner(x):
        return lax.ppermute(x, "ep", [(i, i ^ 1) for i in range(n_ep)])

    wide = moe_tokens.astype(f32)
    local_sq = jnp.sum(wide * wide, axis=1)
    total_sq = sum_ctx(local_sq)
    scale_rows = lax.rsqrt(total_sq / (width * lax.axis_size("ctx")) + norm_eps)
    normed = (wide * scale_rows[:, None] * norm_gain[None, :]).astype(bf16)

    slots = jnp.arange(rows, dtype=jnp.int32)
    pos_right = position(expert_ids, True)
    pos_left = position(expert_ids, False)
    perm_right = (pos_right[None, :] == slots[:, None]).astype(bf16)
    perm_left = (pos_left[None, :] == slots[:, None]).astype(bf16)

    gates = [w_gate[0], partner(w_gate[0])]
    ups = [w_up[0], partner(w_up[0])]
    downs = [w_down[0], partner(w_down[0])]

    held = {}
    for to_right, perm in ((True, perm_right), (False, perm_left)):
        for b, lo, hi in bands:
            block = mm(perm[lo:hi], normed).astype(bf16)
            for k in range(1, nz):
                if to_right:
                    pairs = [(a, a + 1) for a in range(k - 1, nz - 1 - b)]
                else:
                    pairs = [(nz - 1 - a, nz - 2 - a) for a in range(k - 1, nz - 1 - b)]
                if not pairs:
                    break
                block = hop(block, pairs)
                held[to_right, k, b] = block

    def chunk_of(zz, j):
        m = min(zz, nz - 1 - zz)
        if j <= 2 * m:
            return (j % 2 == 1, (j + 1) // 2)
        return (zz > nz - 1 - zz, j - m)

    expert = z

    def picks(ids, scales):
        hits = jnp.any(ids == expert, axis=1)
        at = jnp.arange(rows, dtype=jnp.int32)
        before = hits[None, :] & (at[None, :] < at[:, None])
        slot = jnp.sum(before.astype(jnp.int32), axis=1)
        sel = hits[None, :] & (slot[None, :] == jnp.arange(cap, dtype=jnp.int32)[:, None])
        own = jnp.sum(jnp.where(ids == expert, scales, 0.0), axis=1)
        return sel.astype(bf16), own

    def hidden_of(rows_in, sel):
        parts = jnp.concatenate(
            [mm(rows_in, w) for w in (gates[0], gates[1], ups[0], ups[1])], axis=1
        )
        units = parts.shape[1] // 2

        def act(both):
            return (jax.nn.silu(both[:, :units]) * both[:, units:]).astype(bf16)

        if lax.axis_size("ctx") != 2:
            both = lax.psum_scatter(parts.astype(bf16), "ctx", scatter_dimension=0, tiled=True)
            hid = lax.all_gather(act(both.astype(f32)), "ctx", axis=0, tiled=True)
            return mm_t(sel, hid).astype(bf16)
        theirs = lax.dynamic_slice_in_dim(parts, (1 - ctx) * half, half, 0).astype(bf16)
        mine = lax.dynamic_slice_in_dim(parts, ctx * half, half, 0)
        hid = act(mine + swap_ctx(theirs).astype(f32))
        hid_other = swap_ctx(hid)
        sel_mine = lax.dynamic_slice_in_dim(sel, ctx * half, half, 0)
        sel_other = lax.dynamic_slice_in_dim(sel, (1 - ctx) * half, half, 0)
        return (mm_t(sel_mine, hid) + mm_t(sel_other, hid_other)).astype(bf16)

    fh = w_gate.shape[2]
    step = width // pieces

    def contribution(hid, scale, piece):
        cols = slice(piece * step, (piece + 1) * step)
        out = mm(hid[:, :fh], downs[0][:, cols]) + mm(hid[:, fh:], downs[1][:, cols])
        return out * scale[:, None]

    sel_own, scale_own = picks(expert_ids, route_scale)
    hid_own = hidden_of(mm(sel_own, normed).astype(bf16), sel_own)

    hids = {}
    for j in range(1, nz):
        kinds = [chunk_of(zz, j) for zz in range(nz)]
        distinct = sorted(set(kinds))

        def choose(get):
            value = None
            for kind in distinct:
                here = False
                for zz in range(nz):
                    if kinds[zz] == kind:
                        here = here | (z == zz)
                got = get(kind)
                if got is None:
                    continue
                value = got if value is None else jnp.where(here, got, value)
            return value

        def source_info(kind):
            to_right, k = kind
            return infos[k] if to_right else infos[nz - k]

        chosen = choose(source_info)
        from_left = choose(lambda kind: jnp.full((1,), kind[0], jnp.bool_))[0]
        ids = chosen[:, :top_count].astype(jnp.int32)
        sel, scale = picks(ids, chosen[:, top_count:])
        pos = position(ids, from_left)
        place = (pos[:, None] == slots[None, :]).astype(bf16)
        sel_at = mm(sel, place).astype(bf16)
        scale_at = jnp.sum(jnp.where(pos[:, None] == slots[None, :], scale[:, None], 0.0), axis=0)
        rows_in = None
        for b, lo, hi in bands:
            block = choose(lambda kind: held.get((kind[0], kind[1], b)))
            if block is None:
                continue
            part = mm(sel_at[:, lo:hi], block)
            rows_in = part if rows_in is None else rows_in + part
        hids[j] = (hidden_of(rows_in.astype(bf16), sel_at), scale_at, kinds)

    def chunk_for(to_right, k):
        hid = scale = None
        for j in range(1, nz):
            zs = [zz for zz in range(nz) if hids[j][2][zz] == (to_right, k)]
            if not zs:
                continue
            here = False
            for zz in zs:
                here = here | (z == zz)
            if hid is None:
                hid = jnp.where(here, hids[j][0], 0)
                scale = jnp.where(here, hids[j][1], 0)
            else:
                hid = jnp.where(here, hids[j][0], hid)
                scale = jnp.where(here, hids[j][1], scale)
        return hid, scale

    returned = {}
    for k in range(nz - 1, 0, -1):
        for to_right in (True, False):
            hid, scale = chunk_for(to_right, k)
            for piece in range(pieces):
                acc = contribution(hid, scale, piece)
                for b, lo, hi in bands:
                    value = acc[lo:hi]
                    before = returned.get((to_right, piece, b))
                    if before is not None:
                        value = value + before.astype(f32)
                    pairs = [(a + 1, a) for a in range(k - 1, nz - 1 - b)]
                    if not to_right:
                        pairs = [(nz - 1 - p, nz - 1 - q) for p, q in pairs]
                    if pairs:
                        returned[to_right, piece, b] = hop(value.astype(bf16), pairs)

    outs = []
    for piece in range(pieces):
        acc = contribution(hid_own, scale_own, piece)
        for to_right, perm in ((True, perm_right), (False, perm_left)):
            for b, lo, hi in bands:
                got = returned.get((to_right, piece, b))
                if got is not None:
                    acc = acc + mm_t(perm[lo:hi], got)
        outs.append(acc.astype(bf16))
    moe_out = jnp.concatenate(outs, axis=1)
    attn_out = attention(q_latent, q_rope, latent_keys, rope_keys, w_uv)
    return (attn_out, moe_out)


def expert_kernel(
    nz,
    chunks,
    total_width,
    x_hbm,
    wg_hbm,
    wu_hbm,
    wd_hbm,
    gain_ref,
    route_ref,
    out_hbm,
    xs,
    wgu,
    wd,
    ret,
    con,
    theirs,
    mine,
    outgoing,
    scaled,
    squares,
    squares_in,
    routes,
    local_sem,
    w_send,
    w_recv,
    x_send,
    x_recv,
    r_send,
    r_recv,
    p_send,
    p_recv,
    q_send,
    q_recv,
    t_send,
    t_recv,
    o_sem,
):
    ep = lax.axis_index("ep")
    z = ep // 2
    core = ep % 2
    ctx = lax.axis_index("ctx")
    rows, width = xs.shape[1], xs.shape[2]
    fh = wgu.shape[2]
    groups = rows // 8
    last = nz - 1
    spans = last * chunks
    left, right = {"ep": ep - 2}, {"ep": ep + 2}
    across = {"ctx": 1 - ctx}
    beside = {"ep": 2 * z + 1 - core}

    def remote(src, dst, send, recv, device):
        return pltpu.make_async_remote_copy(
            src_ref=src,
            dst_ref=dst,
            send_sem=send,
            recv_sem=recv,
            device_id=device,
            device_id_type=pl.DeviceIdType.MESH,
        )

    barrier = pltpu.get_barrier_semaphore()
    for step in range(1, nz):
        pl.semaphore_signal(
            barrier,
            inc=1,
            device_id={"ep": 2 * lax.rem(z + step, nz) + core},
            device_id_type=pl.DeviceIdType.MESH,
        )
    for device in (across, beside):
        pl.semaphore_signal(
            barrier, inc=1, device_id=device, device_id_type=pl.DeviceIdType.MESH
        )

    def own_weights(k):
        if k == 0:
            return pltpu.make_async_copy(wg_hbm.at[0], wgu.at[0], local_sem.at[0])
        if k == 1:
            return pltpu.make_async_copy(wu_hbm.at[0], wgu.at[2], local_sem.at[1])
        return pltpu.make_async_copy(wd_hbm.at[0], wd.at[pl.ds(0, fh), :], local_sem.at[2])

    def give_weights(k):
        src = (wg_hbm, wu_hbm, wd_hbm)[k].at[0]
        dst = (wgu.at[1], wgu.at[3], wd.at[pl.ds(fh, fh), :])[k]
        return remote(src, dst, w_send.at[k], w_recv.at[k], beside)

    def own_rows(i):
        return pltpu.make_async_copy(
            x_hbm.at[pl.ds(i * rows, rows), :], xs.at[z * chunks + i], local_sem.at[3 + i]
        )

    def give_rows(i, to_right):
        side = right if to_right else left
        sem = z * chunks + i if to_right else nz * chunks + i
        return remote(
            x_hbm.at[pl.ds(i * rows, rows), :],
            xs.at[z * chunks + i],
            x_send.at[sem],
            x_recv.at[z * chunks + i],
            side,
        )

    def pass_rows(at, to_right):
        side = right if to_right else left
        return remote(xs.at[at], xs.at[at], x_send.at[at], x_recv.at[at], side)

    def give_routes(step):
        to = lax.rem(z + step, nz)
        return remote(
            route_ref.at[to],
            routes.at[z],
            t_send.at[to],
            t_recv.at[z],
            {"ep": 2 * to + core},
        )

    def await_routes(step):
        of = lax.rem(z + step, nz)
        remote(
            route_ref.at[of], routes.at[of], t_send.at[of], t_recv.at[of], {"ep": 2 * of + core}
        ).wait_recv()

    pl.semaphore_wait(barrier, nz + 1)
    for k in range(2):
        own_weights(k).start()
    for i in range(chunks):

        @pl.when(z < last)
        def _():
            give_rows(i, True).start()

        @pl.when(z > 0)
        def _():
            give_rows(i, False).start()

    for step in range(1, nz):
        give_routes(step).start()
    for k in range(2):
        give_weights(k).start()
    own_weights(2).start()
    give_weights(2).start()
    for i in range(chunks):
        own_rows(i).start()
    routes[z] = route_ref[z]

    row_group = lax.broadcasted_iota(jnp.int32, (rows, 128), 0) // 8
    lane = lax.broadcasted_iota(jnp.int32, (rows, 128), 1)
    block = fh if width % fh == 0 else 128

    def spread(packed, offset):
        tall = jnp.broadcast_to(packed[None], (groups, 8, 128)).reshape(rows, 128)
        return jnp.sum(jnp.where(lane == row_group + offset, tall, 0.0), axis=1, keepdims=True)

    def exchange(at, slot):
        return (
            remote(outgoing.at[slot], theirs.at[at], p_send.at[at], p_recv.at[at], across),
            remote(squares.at[slot], squares_in.at[at], q_send.at[at], q_recv.at[at], across),
        )

    def project(at, slot):
        def normalise(n, total):
            cols = pl.ds(pl.multiple_of(n * block, block), block)
            wide = xs[at, :, cols].astype(f32)
            scaled[:, cols] = (wide * gain_ref[:, cols]).astype(bf16)
            square = wide * wide
            for m in range(block // 128):
                total = total + square[:, m * 128 : (m + 1) * 128]
            return total

        total = lax.fori_loop(0, width // block, normalise, jnp.zeros((rows, 128), f32))
        column = jnp.sum(total, axis=1, keepdims=True)
        packed = jnp.where(lane == row_group, jnp.broadcast_to(column, (rows, 128)), 0.0)
        squares[slot] = jnp.sum(packed.reshape(groups, 8, 128), axis=0)

        @pl.loop(0, 4)
        def _(k):
            part = jnp.dot(scaled[...], wgu[k], preferred_element_type=f32)
            mine[slot, k] = part
            outgoing[slot, k] = part.astype(bf16)

        for copy in exchange(at, slot):
            copy.start()

    def expand(source, i, at, slot):
        for copy in exchange(at, slot):
            copy.wait()
        scale = lax.rsqrt(spread(squares[slot] + squares_in[at], 0) / total_width + norm_eps)
        weight = spread(routes[source], i * groups)

        @pl.loop(0, 2)
        def _(b):
            gate = (mine[slot, b] + theirs[at, b].astype(f32)) * scale
            up = (mine[slot, b + 2] + theirs[at, b + 2].astype(f32)) * scale
            hid = jax.nn.silu(gate) * up * weight
            scaled[:, pl.ds(pl.multiple_of(b * fh, fh), fh)] = hid.astype(bf16)

        @pl.loop(0, width // block)
        def _(n):
            cols = pl.ds(pl.multiple_of(n * block, block), block)
            con[at, :, cols] = jnp.dot(
                scaled[:, : 2 * fh], wd[:, cols], preferred_element_type=f32
            ).astype(bf16)

    def place(t, q):
        hop, i = t // chunks, lax.rem(t, chunks)
        source = jnp.where(q == 0, z - 1 - hop, jnp.where(q == 1, z + 1 + hop, z))
        there = (t >= 0) & (t < spans) & (source >= 0) & (source <= last)
        there = there & ((q < 2) | (hop == last - 1))
        return source, i, there

    def give_back(source, i, to_left):
        at = source * chunks + i
        to = at if to_left else at + chunks
        side = left if to_left else right
        return remote(con.at[at], ret.at[to], r_send.at[at], r_recv.at[to], side)

    def await_back(source, i, to_left):
        at = source * chunks + i
        to = at if to_left else at + chunks
        remote(con.at[at], ret.at[to], r_send.at[at], r_recv.at[to], left).wait_recv()
        return to

    def add_back(source, i, tos):
        at = source * chunks + i

        @pl.loop(0, width // block)
        def _(n):
            cols = pl.ds(pl.multiple_of(n * block, block), block)
            value = con[at, :, cols].astype(f32)
            for to in tos:
                value = value + ret[to, :, cols].astype(f32)
            con[at, :, cols] = value.astype(bf16)

    def event(k, near):
        kept = jnp.maximum(near - 1 - SLACK, 0)
        first = chunks - kept
        rest = k - first
        is_first = k < first
        is_mid = rest < (near - 1) * chunks
        hop = jnp.where(is_first, 0, jnp.where(is_mid, 1 + rest // chunks, 0))
        i = jnp.where(
            is_first, k, jnp.where(is_mid, lax.rem(rest, chunks), first + rest - (near - 1) * chunks)
        )
        return hop, i

    def slot_step(t, carry):
        for q, to_right in ((0, True), (1, False)):
            source, i, there = place(t, q)
            onward = (z < last) if to_right else (z > 0)

            @pl.when(there)
            def _():
                at = source * chunks + i
                pass_rows(at, to_right).wait_recv()

                @pl.when(onward)
                def _():
                    pass_rows(at, to_right).start()

        for to_left in (True, False):
            near = z if to_left else last - z
            k = t + 1 - (nz - near) * chunks
            go = (k >= 0) & (k < near * chunks) & (near < last)

            @pl.when(go)
            def _():
                hop, i = event(k, near)
                source = z - 1 - hop if to_left else z + 1 + hop
                to = await_back(source, i, to_left)
                add_back(source, i, [to])
                give_back(source, i, to_left).start()

        @pl.when(t == 0)
        def _():
            for k in range(2):
                own_weights(k).wait()
                give_weights(k).wait()

        @pl.loop(0, 3)
        def _(q):
            source, i, there = place(t, q)

            @pl.when(there)
            def _():
                project(source * chunks + i, lax.rem(t, 2) * 3 + q)

        @pl.when(t == 1)
        def _():
            own_weights(2).wait()
            give_weights(2).wait()
            for step in range(1, nz):
                await_routes(step)

        @pl.loop(0, 3)
        def _(q):
            source, i, there = place(t - 1, q)

            @pl.when(there)
            def _():
                expand(source, i, source * chunks + i, lax.rem(t + 1, 2) * 3 + q)

        for to_left in (True, False):
            near = z if to_left else last - z
            source, i, there = place(t - 1, 0 if to_left else 1)
            kept = jnp.maximum(near - 1 - SLACK, 0)
            held = (t - 1 < chunks) & (i >= chunks - kept)

            @pl.when(there & (near == last) & jnp.logical_not(held))
            def _():
                give_back(source, i, to_left).start()

            @pl.when((near == last) & (t == spans + 1))
            def _():
                for n in range(chunks):

                    @pl.when(n >= chunks - kept)
                    def _():
                        give_back(z - 1 if to_left else z + 1, n, to_left).start()

        return carry

    for i in range(chunks):
        own_rows(i).wait()
    lax.fori_loop(0, nz * chunks, slot_step, 0)

    def finish(i):
        at = z * chunks + i

        @pl.when(z < last)
        def _():
            to = await_back(z, i, True)
            add_back(z, i, [to])

        @pl.when(z > 0)
        def _():
            to = await_back(z, i, False)
            add_back(z, i, [to])

        return pltpu.make_async_copy(
            con.at[at], out_hbm.at[pl.ds(i * rows, rows), :], o_sem.at[i]
        )

    for i in range(chunks):
        finish(i).start()

    for i in range(chunks):
        at = z * chunks + i
        pltpu.make_async_copy(
            con.at[at], out_hbm.at[pl.ds(i * rows, rows), :], o_sem.at[i]
        ).wait()

        @pl.when(z < last)
        def _():
            give_rows(i, True).wait_send()

        @pl.when(z > 0)
        def _():
            give_rows(i, False).wait_send()

    for step in range(1, nz):
        give_routes(step).wait_send()

    def settle(t, carry):
        for q, to_right in ((0, True), (1, False)):
            source, i, there = place(t, q)
            onward = (z < last) if to_right else (z > 0)

            @pl.when(there)
            def _():
                give_back(source, i, to_right).wait_send()

                @pl.when(onward)
                def _():
                    pass_rows(source * chunks + i, to_right).wait_send()

        return carry

    lax.fori_loop(0, spans, settle, 0)


def expert_scratch(nz, rows, width, fh):
    jobs = nz * CHUNKS
    dma = pltpu.SemaphoreType.DMA
    return [
        pltpu.VMEM((jobs, rows, width), bf16),
        pltpu.VMEM((4, width, fh), bf16),
        pltpu.VMEM((2 * fh, width), bf16),
        pltpu.VMEM((jobs + CHUNKS, rows, width), bf16),
        pltpu.VMEM((jobs, rows, width), bf16),
        pltpu.VMEM((jobs, 4, rows, fh), bf16),
        pltpu.VMEM((6, 4, rows, fh), f32),
        pltpu.VMEM((6, 4, rows, fh), bf16),
        pltpu.VMEM((rows, width), bf16),
        pltpu.VMEM((6, 8, 128), f32),
        pltpu.VMEM((jobs, 8, 128), f32),
        pltpu.VMEM((nz, 8, 128), f32),
        dma((3 + CHUNKS,)),
        dma((3,)),
        dma((3,)),
        dma((jobs + CHUNKS,)),
        dma((jobs,)),
        dma((jobs,)),
        dma((jobs + CHUNKS,)),
        dma((jobs,)),
        dma((jobs,)),
        dma((jobs,)),
        dma((jobs,)),
        dma((nz,)),
        dma((nz,)),
        dma((CHUNKS,)),
    ]


def scratch_bytes(shapes):
    total = 0
    for s in shapes:
        if s.memory_space == pltpu.VMEM:
            n = jnp.dtype(s.dtype).itemsize
            for d in s.shape:
                n *= d
            total += n
    return total


def fits(moe_tokens, w_gate):
    n_ep = lax.axis_size("ep")
    nz = n_ep // 2
    tokens, width = moe_tokens.shape
    fh = w_gate.shape[2]
    rows = tokens // CHUNKS
    if lax.axis_size("ctx") != 2 or n_ep % 2 or nz < 2 or w_gate.shape[0] != 1:
        return False
    if tokens % (16 * CHUNKS) or tokens > 1024 or width % 128 or fh % 128:
        return False
    return scratch_bytes(expert_scratch(nz, rows, width, fh)) < VMEM_BYTES - 2**21


def experts(moe_tokens, norm_gain, expert_ids, route_scale, w_gate, w_up, w_down):
    nz = lax.axis_size("ep") // 2
    tokens, width = moe_tokens.shape
    fh = w_gate.shape[2]
    rows = tokens // CHUNKS
    named = expert_ids[None] == jnp.arange(nz, dtype=jnp.int32)[:, None, None]
    table = jnp.sum(jnp.where(named, route_scale[None], 0.0), axis=2)
    table = table.reshape(nz, tokens // 8, 8).transpose(0, 2, 1)
    table = jnp.pad(table, ((0, 0), (0, 0), (0, 128 - tokens // 8)))
    anywhere = pl.BlockSpec(memory_space=pl.ANY)
    whole = pl.BlockSpec(memory_space=pltpu.VMEM)
    return pl.pallas_call(
        functools.partial(expert_kernel, nz, CHUNKS, width * lax.axis_size("ctx")),
        out_shape=jax.ShapeDtypeStruct((tokens, width), bf16),
        in_specs=[anywhere] * 4 + [whole] * 2,
        out_specs=anywhere,
        scratch_shapes=expert_scratch(nz, rows, width, fh),
        compiler_params=pltpu.CompilerParams(
            collective_id=0, has_side_effects=True, vmem_limit_bytes=VMEM_BYTES
        ),
    )(moe_tokens, w_gate, w_up, w_down, norm_gain[None, :], table)


def body(
    q_latent,
    q_rope,
    latent_keys,
    rope_keys,
    w_uv,
    moe_tokens,
    norm_gain,
    expert_ids,
    route_scale,
    w_gate,
    w_up,
    w_down,
):
    if not fits(moe_tokens, w_gate):
        return hop_body(
            q_latent,
            q_rope,
            latent_keys,
            rope_keys,
            w_uv,
            moe_tokens,
            norm_gain,
            expert_ids,
            route_scale,
            w_gate,
            w_up,
            w_down,
        )
    moe_out = experts(moe_tokens, norm_gain, expert_ids, route_scale, w_gate, w_up, w_down)
    attn_out = attention(q_latent, q_rope, latent_keys, rope_keys, w_uv)
    return (attn_out, moe_out)


def solution(mesh):
    return jax.shard_map(
        body,
        mesh=mesh,
        in_specs=(
            P(("group", "ctx"), "ep"),
            P(("group", "ctx"), "ep"),
            P("group", "ctx"),
            P("group", "ctx"),
            P("ep", None, None),
            P(("group", "ep"), "ctx"),
            P("ctx"),
            P(("group", "ep"), None),
            P(("group", "ep"), None),
            P("ep", "ctx", None),
            P("ep", "ctx", None),
            P("ep", None, "ctx"),
        ),
        out_specs=(P(("group", "ctx"), "ep"), P(("group", "ep"), "ctx")),
        check_vma=False,
    )
```

```python
import functools
import jax
import jax.numpy as jnp
from jax import lax
from jax.experimental import pallas as pl
from jax.experimental.pallas import tpu as pltpu
from jax.sharding import PartitionSpec as P

score_scale = 192.0 ** (-0.5)
norm_eps = 1e-06
neg_large = -1e30
PIECES = 2
CHUNKS = 4
VMEM_BYTES = 67043328
f32 = jnp.float32
bf16 = jnp.bfloat16


def mm(a, b):
    return jnp.dot(a, b, preferred_element_type=f32)


def mm_t(a, b):
    return lax.dot_general(a, b, (((0,), (0,)), ((), ())), preferred_element_type=f32)


def swap_ctx(x):
    return lax.ppermute(x, "ctx", [(0, 1), (1, 0)])


def gather_keys(mine, ctx):
    if lax.axis_size("ctx") != 2:
        return lax.all_gather(mine, "ctx", axis=1, tiled=True)
    other = swap_ctx(mine)
    first = ctx == 0
    return jnp.concatenate(
        [jnp.where(first, mine, other), jnp.where(first, other, mine)], axis=1
    )


def sum_ctx(x):
    if lax.axis_size("ctx") != 2:
        return lax.psum(x, "ctx")
    return x + swap_ctx(x)


def attention(q_latent, q_rope, latent_keys, rope_keys, w_uv):
    seq_rows = q_latent.shape[0]
    head_count = w_uv.shape[0]
    latent_dim = latent_keys.shape[0]
    rope_dim = rope_keys.shape[0]
    query_lat = (
        q_latent.reshape(seq_rows, head_count, latent_dim)
        .transpose(1, 0, 2)
        .reshape(head_count * seq_rows, latent_dim)
    )
    query_rot = (
        q_rope.reshape(seq_rows, head_count, rope_dim)
        .transpose(1, 0, 2)
        .reshape(head_count * seq_rows, rope_dim)
    )
    ctx = lax.axis_index("ctx")
    query_pos = ctx * seq_rows + jnp.tile(jnp.arange(seq_rows, dtype=jnp.int32), head_count)
    mine = jnp.concatenate([latent_keys, rope_keys], axis=0)
    keys = gather_keys(mine, ctx)
    lat, rope = keys[:latent_dim], keys[latent_dim:]
    scores = (mm(query_lat, lat) + mm(query_rot, rope)) * score_scale
    key_pos = jnp.arange(lat.shape[1], dtype=jnp.int32)
    visible = key_pos[None, :] <= query_pos[:, None]
    masked = jnp.where(visible, scores, neg_large)
    top = jnp.max(masked, axis=1, keepdims=True)
    weights = jnp.where(visible, jnp.exp(masked - top), 0.0)
    total = jnp.sum(weights, axis=1, keepdims=True)
    update = lax.dot_general(
        weights.astype(bf16), lat, (((1,), (1,)), ((), ())), preferred_element_type=f32
    )
    context = (update / total).astype(bf16).reshape(head_count, seq_rows, latent_dim)
    heads = jnp.einsum("hsl,hlv->shv", context, w_uv, preferred_element_type=f32)
    return heads.reshape(seq_rows, head_count * w_uv.shape[2]).astype(bf16)


def ranks(key):
    n = key.shape[0]
    at = jnp.arange(n, dtype=jnp.int32)
    ahead = (key[None, :] > key[:, None]) | (
        (key[None, :] == key[:, None]) & (at[None, :] < at[:, None])
    )
    return jnp.sum(ahead.astype(jnp.int32), axis=1)


def position(ids, to_right):
    return ranks(jnp.where(to_right, jnp.max(ids, axis=1), -jnp.min(ids, axis=1)))


def hop_body(
    q_latent,
    q_rope,
    latent_keys,
    rope_keys,
    w_uv,
    moe_tokens,
    norm_gain,
    expert_ids,
    route_scale,
    w_gate,
    w_up,
    w_down,
):
    n_ep = lax.axis_size("ep")
    nz = n_ep // 2
    rows, top_count = expert_ids.shape
    cap = min(rows, 3 * rows * top_count // (2 * nz))
    half = cap // 2
    width = moe_tokens.shape[1]
    ep = lax.axis_index("ep")
    z = ep // 2
    ctx = lax.axis_index("ctx")
    group = -(-128 // cap)
    bands = [
        (b, cap * b, min(rows, cap * (b + group)))
        for b in range(0, nz - 1, group)
        if cap * b < rows
    ]
    pieces = max(1, PIECES * width // 3584)

    def hop(x, pairs):
        return lax.ppermute(
            x, "ep", [(2 * a + c, 2 * b + c) for a, b in pairs for c in range(2)]
        )

    info = jnp.concatenate([expert_ids.astype(f32), route_scale], axis=1)
    infos = {0: info}
    for k in range(1, nz):
        infos[k] = hop(info, [(a, (a + k) % nz) for a in range(nz)])

    def partner(x):
        return lax.ppermute(x, "ep", [(i, i ^ 1) for i in range(n_ep)])

    wide = moe_tokens.astype(f32)
    local_sq = jnp.sum(wide * wide, axis=1)
    total_sq = sum_ctx(local_sq)
    scale_rows = lax.rsqrt(total_sq / (width * lax.axis_size("ctx")) + norm_eps)
    normed = (wide * scale_rows[:, None] * norm_gain[None, :]).astype(bf16)

    slots = jnp.arange(rows, dtype=jnp.int32)
    pos_right = position(expert_ids, True)
    pos_left = position(expert_ids, False)
    perm_right = (pos_right[None, :] == slots[:, None]).astype(bf16)
    perm_left = (pos_left[None, :] == slots[:, None]).astype(bf16)

    gates = [w_gate[0], partner(w_gate[0])]
    ups = [w_up[0], partner(w_up[0])]
    downs = [w_down[0], partner(w_down[0])]

    held = {}
    for to_right, perm in ((True, perm_right), (False, perm_left)):
        for b, lo, hi in bands:
            block = mm(perm[lo:hi], normed).astype(bf16)
            for k in range(1, nz):
                if to_right:
                    pairs = [(a, a + 1) for a in range(k - 1, nz - 1 - b)]
                else:
                    pairs = [(nz - 1 - a, nz - 2 - a) for a in range(k - 1, nz - 1 - b)]
                if not pairs:
                    break
                block = hop(block, pairs)
                held[to_right, k, b] = block

    def chunk_of(zz, j):
        m = min(zz, nz - 1 - zz)
        if j <= 2 * m:
            return (j % 2 == 1, (j + 1) // 2)
        return (zz > nz - 1 - zz, j - m)

    expert = z

    def picks(ids, scales):
        hits = jnp.any(ids == expert, axis=1)
        at = jnp.arange(rows, dtype=jnp.int32)
        before = hits[None, :] & (at[None, :] < at[:, None])
        slot = jnp.sum(before.astype(jnp.int32), axis=1)
        sel = hits[None, :] & (slot[None, :] == jnp.arange(cap, dtype=jnp.int32)[:, None])
        own = jnp.sum(jnp.where(ids == expert, scales, 0.0), axis=1)
        return sel.astype(bf16), own

    def hidden_of(rows_in, sel):
        parts = jnp.concatenate(
            [mm(rows_in, w) for w in (gates[0], gates[1], ups[0], ups[1])], axis=1
        )
        units = parts.shape[1] // 2

        def act(both):
            return (jax.nn.silu(both[:, :units]) * both[:, units:]).astype(bf16)

        if lax.axis_size("ctx") != 2:
            both = lax.psum_scatter(parts.astype(bf16), "ctx", scatter_dimension=0, tiled=True)
            hid = lax.all_gather(act(both.astype(f32)), "ctx", axis=0, tiled=True)
            return mm_t(sel, hid).astype(bf16)
        theirs = lax.dynamic_slice_in_dim(parts, (1 - ctx) * half, half, 0).astype(bf16)
        mine = lax.dynamic_slice_in_dim(parts, ctx * half, half, 0)
        hid = act(mine + swap_ctx(theirs).astype(f32))
        hid_other = swap_ctx(hid)
        sel_mine = lax.dynamic_slice_in_dim(sel, ctx * half, half, 0)
        sel_other = lax.dynamic_slice_in_dim(sel, (1 - ctx) * half, half, 0)
        return (mm_t(sel_mine, hid) + mm_t(sel_other, hid_other)).astype(bf16)

    fh = w_gate.shape[2]
    step = width // pieces

    def contribution(hid, scale, piece):
        cols = slice(piece * step, (piece + 1) * step)
        out = mm(hid[:, :fh], downs[0][:, cols]) + mm(hid[:, fh:], downs[1][:, cols])
        return out * scale[:, None]

    sel_own, scale_own = picks(expert_ids, route_scale)
    hid_own = hidden_of(mm(sel_own, normed).astype(bf16), sel_own)

    hids = {}
    for j in range(1, nz):
        kinds = [chunk_of(zz, j) for zz in range(nz)]
        distinct = sorted(set(kinds))

        def choose(get):
            value = None
            for kind in distinct:
                here = False
                for zz in range(nz):
                    if kinds[zz] == kind:
                        here = here | (z == zz)
                got = get(kind)
                if got is None:
                    continue
                value = got if value is None else jnp.where(here, got, value)
            return value

        def source_info(kind):
            to_right, k = kind
            return infos[k] if to_right else infos[nz - k]

        chosen = choose(source_info)
        from_left = choose(lambda kind: jnp.full((1,), kind[0], jnp.bool_))[0]
        ids = chosen[:, :top_count].astype(jnp.int32)
        sel, scale = picks(ids, chosen[:, top_count:])
        pos = position(ids, from_left)
        place = (pos[:, None] == slots[None, :]).astype(bf16)
        sel_at = mm(sel, place).astype(bf16)
        scale_at = jnp.sum(jnp.where(pos[:, None] == slots[None, :], scale[:, None], 0.0), axis=0)
        rows_in = None
        for b, lo, hi in bands:
            block = choose(lambda kind: held.get((kind[0], kind[1], b)))
            if block is None:
                continue
            part = mm(sel_at[:, lo:hi], block)
            rows_in = part if rows_in is None else rows_in + part
        hids[j] = (hidden_of(rows_in.astype(bf16), sel_at), scale_at, kinds)

    def chunk_for(to_right, k):
        hid = scale = None
        for j in range(1, nz):
            zs = [zz for zz in range(nz) if hids[j][2][zz] == (to_right, k)]
            if not zs:
                continue
            here = False
            for zz in zs:
                here = here | (z == zz)
            if hid is None:
                hid = jnp.where(here, hids[j][0], 0)
                scale = jnp.where(here, hids[j][1], 0)
            else:
                hid = jnp.where(here, hids[j][0], hid)
                scale = jnp.where(here, hids[j][1], scale)
        return hid, scale

    returned = {}
    for k in range(nz - 1, 0, -1):
        for to_right in (True, False):
            hid, scale = chunk_for(to_right, k)
            for piece in range(pieces):
                acc = contribution(hid, scale, piece)
                for b, lo, hi in bands:
                    value = acc[lo:hi]
                    before = returned.get((to_right, piece, b))
                    if before is not None:
                        value = value + before.astype(f32)
                    pairs = [(a + 1, a) for a in range(k - 1, nz - 1 - b)]
                    if not to_right:
                        pairs = [(nz - 1 - p, nz - 1 - q) for p, q in pairs]
                    if pairs:
                        returned[to_right, piece, b] = hop(value.astype(bf16), pairs)

    outs = []
    for piece in range(pieces):
        acc = contribution(hid_own, scale_own, piece)
        for to_right, perm in ((True, perm_right), (False, perm_left)):
            for b, lo, hi in bands:
                got = returned.get((to_right, piece, b))
                if got is not None:
                    acc = acc + mm_t(perm[lo:hi], got)
        outs.append(acc.astype(bf16))
    moe_out = jnp.concatenate(outs, axis=1)
    attn_out = attention(q_latent, q_rope, latent_keys, rope_keys, w_uv)
    return (attn_out, moe_out)


def expert_kernel(
    nz,
    chunks,
    total_width,
    ql_hbm,
    qr_hbm,
    lk_hbm,
    rk_hbm,
    uv_hbm,
    x_hbm,
    wg_hbm,
    wu_hbm,
    wd_hbm,
    gain_ref,
    ids_ref,
    scale_ref,
    attn_hbm,
    out_hbm,
    ql,
    qr,
    keys,
    ropes,
    uv,
    attn,
    xs,
    wgu,
    wd,
    ret,
    con,
    theirs,
    mine,
    outgoing,
    scaled,
    squares,
    squares_in,
    table,
    routes,
    a_local,
    a_send,
    a_recv,
    local_sem,
    w_send,
    w_recv,
    x_send,
    x_recv,
    r_send,
    r_recv,
    p_send,
    p_recv,
    q_send,
    q_recv,
    t_send,
    t_recv,
    o_sem,
):
    ep = lax.axis_index("ep")
    z = ep // 2
    core = ep % 2
    ctx = lax.axis_index("ctx")
    rows, width = xs.shape[1], xs.shape[2]
    fh = wgu.shape[2]
    groups = rows // 8
    last = nz - 1
    spans = last * chunks
    half = chunks // 2
    left, right = {"ep": ep - 2}, {"ep": ep + 2}
    across = {"ctx": 1 - ctx}
    beside = {"ep": 2 * z + 1 - core}

    def remote(src, dst, send, recv, device):
        return pltpu.make_async_remote_copy(
            src_ref=src,
            dst_ref=dst,
            send_sem=send,
            recv_sem=recv,
            device_id=device,
            device_id_type=pl.DeviceIdType.MESH,
        )

    barrier = pltpu.get_barrier_semaphore()
    for step in range(1, nz):
        pl.semaphore_signal(
            barrier,
            inc=1,
            device_id={"ep": 2 * lax.rem(z + step, nz) + core},
            device_id_type=pl.DeviceIdType.MESH,
        )
    for device in (across, beside):
        pl.semaphore_signal(
            barrier, inc=1, device_id=device, device_id_type=pl.DeviceIdType.MESH
        )

    def own_weights(k):
        if k == 0:
            return pltpu.make_async_copy(wg_hbm.at[0], wgu.at[0], local_sem.at[0])
        if k == 1:
            return pltpu.make_async_copy(wu_hbm.at[0], wgu.at[2], local_sem.at[1])
        return pltpu.make_async_copy(wd_hbm.at[0], wd.at[pl.ds(0, fh), :], local_sem.at[2])

    def give_weights(k):
        src = (wg_hbm, wu_hbm, wd_hbm)[k].at[0]
        dst = (wgu.at[1], wgu.at[3], wd.at[pl.ds(fh, fh), :])[k]
        return remote(src, dst, w_send.at[k], w_recv.at[k], beside)

    def own_rows(i):
        return pltpu.make_async_copy(
            x_hbm.at[pl.ds(i * rows, rows), :], xs.at[z * chunks + i], local_sem.at[3 + i]
        )

    def give_rows(i, to_right):
        side = right if to_right else left
        sem = z * chunks + i if to_right else nz * chunks + i
        return remote(
            x_hbm.at[pl.ds(i * rows, rows), :],
            xs.at[z * chunks + i],
            x_send.at[sem],
            x_recv.at[z * chunks + i],
            side,
        )

    def pass_rows(at, to_right):
        side = right if to_right else left
        return remote(xs.at[at], xs.at[at], x_send.at[at], x_recv.at[at], side)

    def give_routes(step):
        to = lax.rem(z + step, nz)
        return remote(
            table.at[to],
            routes.at[z],
            t_send.at[to],
            t_recv.at[z],
            {"ep": 2 * to + core},
        )

    def await_routes(step):
        of = lax.rem(z + step, nz)
        remote(
            table.at[of], routes.at[of], t_send.at[of], t_recv.at[of], {"ep": 2 * of + core}
        ).wait_recv()

    seq = ql.shape[0]
    latent = keys.shape[0]
    turn = qr_hbm.shape[1] // uv.shape[0]
    mine_at = pl.ds(pl.multiple_of(ctx * seq, seq), seq)
    key_parts = (
        (lk_hbm, keys.at[:, mine_at]),
        (rk_hbm, ropes.at[0, pl.ds(0, turn), mine_at]),
        (rk_hbm, ropes.at[1, pl.ds(turn, turn), mine_at]),
    )

    def local_attention():
        pairs = key_parts + ((ql_hbm, ql), (qr_hbm, qr), (uv_hbm, uv))
        return [
            pltpu.make_async_copy(src, dst, a_local.at[n]) for n, (src, dst) in enumerate(pairs)
        ]

    def give_keys():
        return [
            remote(src, dst, a_send.at[n], a_recv.at[n], across)
            for n, (src, dst) in enumerate(key_parts)
        ]

    def put_attention():
        return pltpu.make_async_copy(attn, attn_hbm, a_local.at[6])

    def attend(head):
        span = keys.shape[1]
        value = uv.shape[2]
        pair = head // 2
        query = ctx * seq + lax.broadcasted_iota(jnp.int32, (seq, span), 0)
        visible = lax.broadcasted_iota(jnp.int32, (seq, span), 1) <= query
        query_lat = ql[:, pl.ds(pl.multiple_of(head * latent, latent), latent)]
        query_rot = qr[:, pl.ds(pl.multiple_of(pair * 2 * turn, 2 * turn), 2 * turn)]
        rotary = ropes[lax.rem(head, 2)]
        scores = (mm(query_lat, keys[...]) + mm(query_rot, rotary)) * score_scale
        masked = jnp.where(visible, scores, neg_large)
        top = jnp.max(masked, axis=1, keepdims=True)
        weights = jnp.where(visible, jnp.exp(masked - top), 0.0)
        whole = jnp.sum(weights, axis=1, keepdims=True)
        update = lax.dot_general(
            weights.astype(bf16), keys[...], (((1,), (1,)), ((), ())), preferred_element_type=f32
        )
        attn[:, pl.ds(pl.multiple_of(head * value, value), value)] = mm(
            (update / whole).astype(bf16), uv[head]
        ).astype(bf16)

    for copy in local_attention():
        copy.start()
    ropes[0, turn:, :] = jnp.zeros((turn, ropes.shape[2]), bf16)
    ropes[1, :turn, :] = jnp.zeros((turn, ropes.shape[2]), bf16)
    for expert in range(nz):
        line = jnp.zeros((1, table.shape[2]), f32)
        for k in range(ids_ref.shape[0]):
            line = line + jnp.where(
                ids_ref[k : k + 1, :] == expert, scale_ref[k : k + 1, :], 0.0
            )
        table[expert] = jnp.broadcast_to(line, table.shape[1:])
    pl.semaphore_wait(barrier, nz + 1)
    for k in range(2):
        own_weights(k).start()
    for i in range(half):

        @pl.when(z < last)
        def _():
            give_rows(i, True).start()

        @pl.when(z > 0)
        def _():
            give_rows(i, False).start()

    def give_rest(to_right):
        for i in range(half, chunks):
            give_rows(i, to_right).start()

    @pl.when(z == 0)
    def _():
        give_rest(True)

    @pl.when(z == last)
    def _():
        give_rest(False)

    for copy in give_keys():
        copy.start()
    for k in range(2):
        give_weights(k).start()
    own_weights(2).start()
    give_weights(2).start()
    for i in range(chunks):
        own_rows(i).start()
    routes[z] = table[z]
    for step in range(1, nz):
        give_routes(step).start()

    row_group = lax.broadcasted_iota(jnp.int32, (rows, 128), 0) // 8
    lane = lax.broadcasted_iota(jnp.int32, (rows, 128), 1)
    block = fh if width % fh == 0 else 128

    def spread(packed):
        tall = jnp.broadcast_to(packed[None], (groups, 8, 128)).reshape(rows, 128)
        return jnp.sum(jnp.where(lane == row_group, tall, 0.0), axis=1, keepdims=True)

    def weights_of(source, i):
        tokens = routes.shape[2]
        shape = (rows, tokens)
        wanted = lax.broadcasted_iota(jnp.int32, shape, 0) + i * rows
        hit = lax.broadcasted_iota(jnp.int32, shape, 1) == wanted
        line = jnp.broadcast_to(routes[source][0:1, :], shape)
        return jnp.sum(jnp.where(hit, line, 0.0), axis=1, keepdims=True)

    def exchange(at, slot):
        return (
            remote(outgoing.at[slot], theirs.at[at], p_send.at[at], p_recv.at[at], across),
            remote(squares.at[slot], squares_in.at[at], q_send.at[at], q_recv.at[at], across),
        )

    def project(at, slot):
        def normalise(n, total):
            cols = pl.ds(pl.multiple_of(n * block, block), block)
            wide = xs[at, :, cols].astype(f32)
            scaled[:, cols] = (wide * gain_ref[cols][None, :]).astype(bf16)
            square = wide * wide
            for m in range(block // 128):
                total = total + square[:, m * 128 : (m + 1) * 128]
            return total

        total = lax.fori_loop(0, width // block, normalise, jnp.zeros((rows, 128), f32))
        column = jnp.sum(total, axis=1, keepdims=True)
        packed = jnp.where(lane == row_group, jnp.broadcast_to(column, (rows, 128)), 0.0)
        squares[slot] = jnp.sum(packed.reshape(groups, 8, 128), axis=0)

        @pl.loop(0, 4)
        def _(k):
            part = jnp.dot(scaled[...], wgu[k], preferred_element_type=f32)
            mine[slot, k] = part
            outgoing[slot, k] = part.astype(bf16)

        for copy in exchange(at, slot):
            copy.start()

    def expand(source, i, at, slot):
        for copy in exchange(at, slot):
            copy.wait()
        scale = lax.rsqrt(spread(squares[slot] + squares_in[at]) / total_width + norm_eps)
        weight = weights_of(source, i)

        @pl.loop(0, 2)
        def _(b):
            gate = (mine[slot, b] + theirs[at, b].astype(f32)) * scale
            up = (mine[slot, b + 2] + theirs[at, b + 2].astype(f32)) * scale
            hid = jax.nn.silu(gate) * up * weight
            scaled[:, pl.ds(pl.multiple_of(b * fh, fh), fh)] = hid.astype(bf16)

        @pl.loop(0, width // block)
        def _(n):
            cols = pl.ds(pl.multiple_of(n * block, block), block)
            con[at, :, cols] = jnp.dot(
                scaled[:, : 2 * fh], wd[:, cols], preferred_element_type=f32
            ).astype(bf16)

    def arrival(k, from_left):
        near = z if from_left else last - z
        part = k // half
        late = part >= near
        source = jnp.where(late, part - near, near - 1 - part)
        i = lax.rem(k, half) + jnp.where(late, half, 0)
        there = (k >= 0) & (k < near * chunks)
        return source if from_left else last - source, i, there

    def place(t, q):
        left_source, left_i, left_there = arrival(t, True)
        right_source, right_i, right_there = arrival(t, False)
        own_i = t - (spans - chunks)
        own_there = (own_i >= 0) & (own_i < chunks)
        source = jnp.where(q == 0, left_source, jnp.where(q == 1, right_source, z))
        i = jnp.where(q == 0, left_i, jnp.where(q == 1, right_i, own_i))
        there = ((q == 0) & left_there) | ((q == 1) & right_there) | ((q == 2) & own_there)
        return source, i, there

    def give_back(source, i, to_left):
        at = source * chunks + i
        to = at if to_left else at + chunks
        side = left if to_left else right
        return remote(con.at[at], ret.at[to], r_send.at[at], r_recv.at[to], side)

    def await_back(source, i, to_left):
        at = source * chunks + i
        to = at if to_left else at + chunks
        remote(con.at[at], ret.at[to], r_send.at[at], r_recv.at[to], left).wait_recv()
        return to

    def add_back(source, i, tos):
        at = source * chunks + i

        @pl.loop(0, width // block)
        def _(n):
            cols = pl.ds(pl.multiple_of(n * block, block), block)
            value = con[at, :, cols].astype(f32)
            for to in tos:
                value = value + ret[to, :, cols].astype(f32)
            con[at, :, cols] = value.astype(bf16)

    def slot_step(t, carry):
        for to_right in (True, False):
            source, i, there = arrival(t, to_right)
            onward = (z < last) if to_right else (z > 0)
            near = z if to_right else last - z

            @pl.when(there)
            def _():
                at = source * chunks + i
                pass_rows(at, to_right).wait_recv()

                @pl.when(onward)
                def _():
                    pass_rows(at, to_right).start()

            @pl.when(onward & (near > 0) & (t == near * chunks - 1))
            def _():
                give_rest(to_right)

        @pl.when(t == 0)
        def _():
            for k in range(2):
                own_weights(k).wait()
                give_weights(k).wait()

        @pl.loop(0, 3)
        def _(q):
            source, i, there = place(t, q)

            @pl.when(there)
            def _():
                project(source * chunks + i, lax.rem(t, 2) * 3 + q)

        @pl.when(t == 1)
        def _():
            own_weights(2).wait()
            give_weights(2).wait()
            for step in range(1, nz):
                await_routes(step)

        heads = uv.shape[0]

        @pl.when(t == chunks)
        def _():
            for copy in local_attention():
                copy.wait()
            for copy in give_keys():
                copy.wait()

        @pl.when((t >= chunks) & (t < chunks + heads))
        def _():
            attend(t - chunks)

        @pl.when(t == chunks + heads)
        def _():
            put_attention().start()

        @pl.loop(0, 3)
        def _(q):
            source, i, there = place(t - 1, q)

            @pl.when(there)
            def _():
                expand(source, i, source * chunks + i, lax.rem(t + 1, 2) * 3 + q)

        for to_left in (True, False):
            near = z if to_left else last - z
            source, i, there = arrival(t - 1, to_left)

            @pl.when(there & (near == last))
            def _():
                give_back(source, i, to_left).start()

            k = t + half - (nz - near) * chunks
            source_back, i_back, there_back = arrival(k, to_left)

            @pl.when(there_back & (near < last))
            def _():
                to = await_back(source_back, i_back, to_left)
                add_back(source_back, i_back, [to])
                give_back(source_back, i_back, to_left).start()

        return carry

    for i in range(chunks):
        own_rows(i).wait()
    lax.fori_loop(0, nz * chunks, slot_step, 0)

    def finish(i):
        at = z * chunks + i

        @pl.when(z < last)
        def _():
            to = await_back(z, i, True)
            add_back(z, i, [to])

        @pl.when(z > 0)
        def _():
            to = await_back(z, i, False)
            add_back(z, i, [to])

        return pltpu.make_async_copy(
            con.at[at], out_hbm.at[pl.ds(i * rows, rows), :], o_sem.at[i]
        )

    for i in range(chunks):
        finish(i).start()

    put_attention().wait()
    for i in range(chunks):
        at = z * chunks + i
        pltpu.make_async_copy(
            con.at[at], out_hbm.at[pl.ds(i * rows, rows), :], o_sem.at[i]
        ).wait()

        @pl.when(z < last)
        def _():
            give_rows(i, True).wait_send()

        @pl.when(z > 0)
        def _():
            give_rows(i, False).wait_send()

    for step in range(1, nz):
        give_routes(step).wait_send()

    def settle(t, carry):
        for to_right in (True, False):
            source, i, there = arrival(t, to_right)
            onward = (z < last) if to_right else (z > 0)

            @pl.when(there)
            def _():
                give_back(source, i, to_right).wait_send()

                @pl.when(onward)
                def _():
                    pass_rows(source * chunks + i, to_right).wait_send()

        return carry

    lax.fori_loop(0, spans, settle, 0)


def expert_scratch(nz, rows, width, fh, seq, heads, latent, turn, value, tokens):
    jobs = nz * CHUNKS
    dma = pltpu.SemaphoreType.DMA
    return [
        pltpu.VMEM((seq, heads * latent), bf16),
        pltpu.VMEM((seq, heads * turn), bf16),
        pltpu.VMEM((latent, 2 * seq), bf16),
        pltpu.VMEM((2, 2 * turn, 2 * seq), bf16),
        pltpu.VMEM((heads, latent, value), bf16),
        pltpu.VMEM((seq, heads * value), bf16),
        pltpu.VMEM((jobs, rows, width), bf16),
        pltpu.VMEM((4, width, fh), bf16),
        pltpu.VMEM((2 * fh, width), bf16),
        pltpu.VMEM((jobs + CHUNKS, rows, width), bf16),
        pltpu.VMEM((jobs, rows, width), bf16),
        pltpu.VMEM((jobs, 4, rows, fh), bf16),
        pltpu.VMEM((6, 4, rows, fh), f32),
        pltpu.VMEM((6, 4, rows, fh), bf16),
        pltpu.VMEM((rows, width), bf16),
        pltpu.VMEM((6, 8, 128), f32),
        pltpu.VMEM((jobs, 8, 128), f32),
        pltpu.VMEM((nz, 8, tokens), f32),
        pltpu.VMEM((nz, 8, tokens), f32),
        dma((7,)),
        dma((3,)),
        dma((3,)),
        dma((3 + CHUNKS,)),
        dma((3,)),
        dma((3,)),
        dma((jobs + CHUNKS,)),
        dma((jobs,)),
        dma((jobs,)),
        dma((jobs + CHUNKS,)),
        dma((jobs,)),
        dma((jobs,)),
        dma((jobs,)),
        dma((jobs,)),
        dma((nz,)),
        dma((nz,)),
        dma((CHUNKS,)),
    ]


def scratch_bytes(shapes):
    total = 0
    for s in shapes:
        if s.memory_space == pltpu.VMEM:
            n = jnp.dtype(s.dtype).itemsize
            for d in s.shape:
                n *= d
            total += n
    return total


def sizes(latent_keys, rope_keys, w_uv, moe_tokens, w_gate):
    heads, latent, value = w_uv.shape
    tokens, width = moe_tokens.shape
    return dict(
        nz=lax.axis_size("ep") // 2,
        rows=tokens // CHUNKS,
        width=width,
        fh=w_gate.shape[2],
        seq=latent_keys.shape[1],
        heads=heads,
        latent=latent,
        turn=rope_keys.shape[0],
        value=value,
        tokens=tokens,
    )


def fits(n, w_gate):
    n_ep = lax.axis_size("ep")
    if lax.axis_size("ctx") != 2 or n_ep % 2 or n["nz"] < 2 or w_gate.shape[0] != 1:
        return False
    if n["tokens"] % (16 * CHUNKS) or n["rows"] > 1024 or n["heads"] > (n["nz"] - 1) * CHUNKS:
        return False
    lanes = ("width", "fh", "seq", "latent", "value", "tokens")
    if any(n[name] % 128 for name in lanes) or n["turn"] != 64 or n["heads"] % 2:
        return False
    return scratch_bytes(expert_scratch(**n)) < VMEM_BYTES - 2**20


def fused(n, attention_in, moe_in):
    moe_tokens, norm_gain, expert_ids, route_scale, w_gate, w_up, w_down = moe_in
    anywhere = pl.BlockSpec(memory_space=pl.ANY)
    whole = pl.BlockSpec(memory_space=pltpu.VMEM)
    total = n["width"] * lax.axis_size("ctx")
    return pl.pallas_call(
        functools.partial(expert_kernel, n["nz"], CHUNKS, total),
        out_shape=(
            jax.ShapeDtypeStruct((n["seq"], n["heads"] * n["value"]), bf16),
            jax.ShapeDtypeStruct((n["tokens"], n["width"]), bf16),
        ),
        in_specs=[anywhere] * 9 + [whole] * 3,
        out_specs=(anywhere, anywhere),
        scratch_shapes=expert_scratch(**n),
        compiler_params=pltpu.CompilerParams(
            collective_id=0, has_side_effects=True, vmem_limit_bytes=VMEM_BYTES
        ),
    )(*attention_in, moe_tokens, w_gate, w_up, w_down, norm_gain, expert_ids.T, route_scale.T)


def body(
    q_latent,
    q_rope,
    latent_keys,
    rope_keys,
    w_uv,
    moe_tokens,
    norm_gain,
    expert_ids,
    route_scale,
    w_gate,
    w_up,
    w_down,
):
    n = sizes(latent_keys, rope_keys, w_uv, moe_tokens, w_gate)
    if not fits(n, w_gate):
        return hop_body(
            q_latent,
            q_rope,
            latent_keys,
            rope_keys,
            w_uv,
            moe_tokens,
            norm_gain,
            expert_ids,
            route_scale,
            w_gate,
            w_up,
            w_down,
        )
    attention_in = (q_latent, q_rope, latent_keys, rope_keys, w_uv)
    moe_in = (moe_tokens, norm_gain, expert_ids, route_scale, w_gate, w_up, w_down)
    return fused(n, attention_in, moe_in)


def solution(mesh):
    return jax.shard_map(
        body,
        mesh=mesh,
        in_specs=(
            P(("group", "ctx"), "ep"),
            P(("group", "ctx"), "ep"),
            P("group", "ctx"),
            P("group", "ctx"),
            P("ep", None, None),
            P(("group", "ep"), "ctx"),
            P("ctx"),
            P(("group", "ep"), None),
            P(("group", "ep"), None),
            P("ep", "ctx", None),
            P("ep", "ctx", None),
            P("ep", None, "ctx"),
        ),
        out_specs=(P(("group", "ctx"), "ep"), P(("group", "ep"), "ctx")),
        check_vma=False,
    )
```

```python
import functools
import jax
import jax.numpy as jnp
from jax import lax
from jax.experimental import pallas as pl
from jax.experimental.pallas import tpu as pltpu
from jax.sharding import PartitionSpec as P

score_scale = 192.0 ** (-0.5)
norm_eps = 1e-06
neg_large = -1e30
PIECES = 2
CHUNKS = 4
LAG = 2
STEPS = 2
VMEM_BYTES = 67043328
f32 = jnp.float32
bf16 = jnp.bfloat16


def mm(a, b):
    return jnp.dot(a, b, preferred_element_type=f32)


def mm_t(a, b):
    return lax.dot_general(a, b, (((0,), (0,)), ((), ())), preferred_element_type=f32)


def swap_ctx(x):
    return lax.ppermute(x, "ctx", [(0, 1), (1, 0)])


def gather_keys(mine, ctx):
    if lax.axis_size("ctx") != 2:
        return lax.all_gather(mine, "ctx", axis=1, tiled=True)
    other = swap_ctx(mine)
    first = ctx == 0
    return jnp.concatenate(
        [jnp.where(first, mine, other), jnp.where(first, other, mine)], axis=1
    )


def sum_ctx(x):
    if lax.axis_size("ctx") != 2:
        return lax.psum(x, "ctx")
    return x + swap_ctx(x)


def attention(q_latent, q_rope, latent_keys, rope_keys, w_uv):
    seq_rows = q_latent.shape[0]
    head_count = w_uv.shape[0]
    latent_dim = latent_keys.shape[0]
    rope_dim = rope_keys.shape[0]
    query_lat = (
        q_latent.reshape(seq_rows, head_count, latent_dim)
        .transpose(1, 0, 2)
        .reshape(head_count * seq_rows, latent_dim)
    )
    query_rot = (
        q_rope.reshape(seq_rows, head_count, rope_dim)
        .transpose(1, 0, 2)
        .reshape(head_count * seq_rows, rope_dim)
    )
    ctx = lax.axis_index("ctx")
    query_pos = ctx * seq_rows + jnp.tile(jnp.arange(seq_rows, dtype=jnp.int32), head_count)
    mine = jnp.concatenate([latent_keys, rope_keys], axis=0)
    keys = gather_keys(mine, ctx)
    lat, rope = keys[:latent_dim], keys[latent_dim:]
    scores = (mm(query_lat, lat) + mm(query_rot, rope)) * score_scale
    key_pos = jnp.arange(lat.shape[1], dtype=jnp.int32)
    visible = key_pos[None, :] <= query_pos[:, None]
    masked = jnp.where(visible, scores, neg_large)
    top = jnp.max(masked, axis=1, keepdims=True)
    weights = jnp.where(visible, jnp.exp(masked - top), 0.0)
    total = jnp.sum(weights, axis=1, keepdims=True)
    update = lax.dot_general(
        weights.astype(bf16), lat, (((1,), (1,)), ((), ())), preferred_element_type=f32
    )
    context = (update / total).astype(bf16).reshape(head_count, seq_rows, latent_dim)
    heads = jnp.einsum("hsl,hlv->shv", context, w_uv, preferred_element_type=f32)
    return heads.reshape(seq_rows, head_count * w_uv.shape[2]).astype(bf16)


def ranks(key):
    n = key.shape[0]
    at = jnp.arange(n, dtype=jnp.int32)
    ahead = (key[None, :] > key[:, None]) | (
        (key[None, :] == key[:, None]) & (at[None, :] < at[:, None])
    )
    return jnp.sum(ahead.astype(jnp.int32), axis=1)


def position(ids, to_right):
    return ranks(jnp.where(to_right, jnp.max(ids, axis=1), -jnp.min(ids, axis=1)))


def hop_body(
    q_latent,
    q_rope,
    latent_keys,
    rope_keys,
    w_uv,
    moe_tokens,
    norm_gain,
    expert_ids,
    route_scale,
    w_gate,
    w_up,
    w_down,
):
    n_ep = lax.axis_size("ep")
    nz = n_ep // 2
    rows, top_count = expert_ids.shape
    cap = min(rows, 3 * rows * top_count // (2 * nz))
    half = cap // 2
    width = moe_tokens.shape[1]
    ep = lax.axis_index("ep")
    z = ep // 2
    ctx = lax.axis_index("ctx")
    group = -(-128 // cap)
    bands = [
        (b, cap * b, min(rows, cap * (b + group)))
        for b in range(0, nz - 1, group)
        if cap * b < rows
    ]
    pieces = max(1, PIECES * width // 3584)

    def hop(x, pairs):
        return lax.ppermute(
            x, "ep", [(2 * a + c, 2 * b + c) for a, b in pairs for c in range(2)]
        )

    info = jnp.concatenate([expert_ids.astype(f32), route_scale], axis=1)
    infos = {0: info}
    for k in range(1, nz):
        infos[k] = hop(info, [(a, (a + k) % nz) for a in range(nz)])

    def partner(x):
        return lax.ppermute(x, "ep", [(i, i ^ 1) for i in range(n_ep)])

    wide = moe_tokens.astype(f32)
    local_sq = jnp.sum(wide * wide, axis=1)
    total_sq = sum_ctx(local_sq)
    scale_rows = lax.rsqrt(total_sq / (width * lax.axis_size("ctx")) + norm_eps)
    normed = (wide * scale_rows[:, None] * norm_gain[None, :]).astype(bf16)

    slots = jnp.arange(rows, dtype=jnp.int32)
    pos_right = position(expert_ids, True)
    pos_left = position(expert_ids, False)
    perm_right = (pos_right[None, :] == slots[:, None]).astype(bf16)
    perm_left = (pos_left[None, :] == slots[:, None]).astype(bf16)

    gates = [w_gate[0], partner(w_gate[0])]
    ups = [w_up[0], partner(w_up[0])]
    downs = [w_down[0], partner(w_down[0])]

    held = {}
    for to_right, perm in ((True, perm_right), (False, perm_left)):
        for b, lo, hi in bands:
            block = mm(perm[lo:hi], normed).astype(bf16)
            for k in range(1, nz):
                if to_right:
                    pairs = [(a, a + 1) for a in range(k - 1, nz - 1 - b)]
                else:
                    pairs = [(nz - 1 - a, nz - 2 - a) for a in range(k - 1, nz - 1 - b)]
                if not pairs:
                    break
                block = hop(block, pairs)
                held[to_right, k, b] = block

    def chunk_of(zz, j):
        m = min(zz, nz - 1 - zz)
        if j <= 2 * m:
            return (j % 2 == 1, (j + 1) // 2)
        return (zz > nz - 1 - zz, j - m)

    expert = z

    def picks(ids, scales):
        hits = jnp.any(ids == expert, axis=1)
        at = jnp.arange(rows, dtype=jnp.int32)
        before = hits[None, :] & (at[None, :] < at[:, None])
        slot = jnp.sum(before.astype(jnp.int32), axis=1)
        sel = hits[None, :] & (slot[None, :] == jnp.arange(cap, dtype=jnp.int32)[:, None])
        own = jnp.sum(jnp.where(ids == expert, scales, 0.0), axis=1)
        return sel.astype(bf16), own

    def hidden_of(rows_in, sel):
        parts = jnp.concatenate(
            [mm(rows_in, w) for w in (gates[0], gates[1], ups[0], ups[1])], axis=1
        )
        units = parts.shape[1] // 2

        def act(both):
            return (jax.nn.silu(both[:, :units]) * both[:, units:]).astype(bf16)

        if lax.axis_size("ctx") != 2:
            both = lax.psum_scatter(parts.astype(bf16), "ctx", scatter_dimension=0, tiled=True)
            hid = lax.all_gather(act(both.astype(f32)), "ctx", axis=0, tiled=True)
            return mm_t(sel, hid).astype(bf16)
        theirs = lax.dynamic_slice_in_dim(parts, (1 - ctx) * half, half, 0).astype(bf16)
        mine = lax.dynamic_slice_in_dim(parts, ctx * half, half, 0)
        hid = act(mine + swap_ctx(theirs).astype(f32))
        hid_other = swap_ctx(hid)
        sel_mine = lax.dynamic_slice_in_dim(sel, ctx * half, half, 0)
        sel_other = lax.dynamic_slice_in_dim(sel, (1 - ctx) * half, half, 0)
        return (mm_t(sel_mine, hid) + mm_t(sel_other, hid_other)).astype(bf16)

    fh = w_gate.shape[2]
    step = width // pieces

    def contribution(hid, scale, piece):
        cols = slice(piece * step, (piece + 1) * step)
        out = mm(hid[:, :fh], downs[0][:, cols]) + mm(hid[:, fh:], downs[1][:, cols])
        return out * scale[:, None]

    sel_own, scale_own = picks(expert_ids, route_scale)
    hid_own = hidden_of(mm(sel_own, normed).astype(bf16), sel_own)

    hids = {}
    for j in range(1, nz):
        kinds = [chunk_of(zz, j) for zz in range(nz)]
        distinct = sorted(set(kinds))

        def choose(get):
            value = None
            for kind in distinct:
                here = False
                for zz in range(nz):
                    if kinds[zz] == kind:
                        here = here | (z == zz)
                got = get(kind)
                if got is None:
                    continue
                value = got if value is None else jnp.where(here, got, value)
            return value

        def source_info(kind):
            to_right, k = kind
            return infos[k] if to_right else infos[nz - k]

        chosen = choose(source_info)
        from_left = choose(lambda kind: jnp.full((1,), kind[0], jnp.bool_))[0]
        ids = chosen[:, :top_count].astype(jnp.int32)
        sel, scale = picks(ids, chosen[:, top_count:])
        pos = position(ids, from_left)
        place = (pos[:, None] == slots[None, :]).astype(bf16)
        sel_at = mm(sel, place).astype(bf16)
        scale_at = jnp.sum(jnp.where(pos[:, None] == slots[None, :], scale[:, None], 0.0), axis=0)
        rows_in = None
        for b, lo, hi in bands:
            block = choose(lambda kind: held.get((kind[0], kind[1], b)))
            if block is None:
                continue
            part = mm(sel_at[:, lo:hi], block)
            rows_in = part if rows_in is None else rows_in + part
        hids[j] = (hidden_of(rows_in.astype(bf16), sel_at), scale_at, kinds)

    def chunk_for(to_right, k):
        hid = scale = None
        for j in range(1, nz):
            zs = [zz for zz in range(nz) if hids[j][2][zz] == (to_right, k)]
            if not zs:
                continue
            here = False
            for zz in zs:
                here = here | (z == zz)
            if hid is None:
                hid = jnp.where(here, hids[j][0], 0)
                scale = jnp.where(here, hids[j][1], 0)
            else:
                hid = jnp.where(here, hids[j][0], hid)
                scale = jnp.where(here, hids[j][1], scale)
        return hid, scale

    returned = {}
    for k in range(nz - 1, 0, -1):
        for to_right in (True, False):
            hid, scale = chunk_for(to_right, k)
            for piece in range(pieces):
                acc = contribution(hid, scale, piece)
                for b, lo, hi in bands:
                    value = acc[lo:hi]
                    before = returned.get((to_right, piece, b))
                    if before is not None:
                        value = value + before.astype(f32)
                    pairs = [(a + 1, a) for a in range(k - 1, nz - 1 - b)]
                    if not to_right:
                        pairs = [(nz - 1 - p, nz - 1 - q) for p, q in pairs]
                    if pairs:
                        returned[to_right, piece, b] = hop(value.astype(bf16), pairs)

    outs = []
    for piece in range(pieces):
        acc = contribution(hid_own, scale_own, piece)
        for to_right, perm in ((True, perm_right), (False, perm_left)):
            for b, lo, hi in bands:
                got = returned.get((to_right, piece, b))
                if got is not None:
                    acc = acc + mm_t(perm[lo:hi], got)
        outs.append(acc.astype(bf16))
    moe_out = jnp.concatenate(outs, axis=1)
    attn_out = attention(q_latent, q_rope, latent_keys, rope_keys, w_uv)
    return (attn_out, moe_out)


def expert_kernel(
    nz,
    chunks,
    total_width,
    ql_hbm,
    qr_hbm,
    lk_hbm,
    rk_hbm,
    uv_hbm,
    x_hbm,
    wg_hbm,
    wu_hbm,
    wd_hbm,
    gain_ref,
    ids_ref,
    scale_ref,
    attn_hbm,
    own_hbm,
    right_hbm,
    left_hbm,
    ql,
    qr,
    keys,
    ropes,
    uv,
    attn,
    xs,
    wgu,
    wd,
    ret,
    con,
    theirs,
    mine,
    outgoing,
    scaled,
    squares,
    squares_in,
    routes,
    a_local,
    a_send,
    a_recv,
    local_sem,
    w_send,
    w_recv,
    x_send,
    x_recv,
    r_send,
    r_recv,
    p_send,
    p_recv,
    q_send,
    q_recv,
    t_send,
    t_recv,
    o_sem,
):
    ep = lax.axis_index("ep")
    z = ep // 2
    core = ep % 2
    ctx = lax.axis_index("ctx")
    rows, width = xs.shape[1], xs.shape[2]
    fh = wgu.shape[2]
    groups = rows // 8
    last = nz - 1
    spans = last * chunks
    half = chunks // 2
    left, right = {"ep": ep - 2}, {"ep": ep + 2}
    across = {"ctx": 1 - ctx}
    beside = {"ep": 2 * z + 1 - core}

    def remote(src, dst, send, recv, device):
        return pltpu.make_async_remote_copy(
            src_ref=src,
            dst_ref=dst,
            send_sem=send,
            recv_sem=recv,
            device_id=device,
            device_id_type=pl.DeviceIdType.MESH,
        )

    barrier = pltpu.get_barrier_semaphore()
    for near, device in ((z > 0, left), (z < last, right)):

        @pl.when(near)
        def _():
            pl.semaphore_signal(
                barrier, inc=1, device_id=device, device_id_type=pl.DeviceIdType.MESH
            )

    for device in (across, beside):
        pl.semaphore_signal(
            barrier, inc=1, device_id=device, device_id_type=pl.DeviceIdType.MESH
        )

    def own_weights(k):
        if k == 0:
            return pltpu.make_async_copy(wg_hbm.at[0], wgu.at[0], local_sem.at[0])
        if k == 1:
            return pltpu.make_async_copy(wu_hbm.at[0], wgu.at[2], local_sem.at[1])
        return pltpu.make_async_copy(wd_hbm.at[0], wd.at[pl.ds(0, fh), :], local_sem.at[2])

    def give_weights(k):
        src = (wg_hbm, wu_hbm, wd_hbm)[k].at[0]
        dst = (wgu.at[1], wgu.at[3], wd.at[pl.ds(fh, fh), :])[k]
        return remote(src, dst, w_send.at[k], w_recv.at[k], beside)

    def own_rows(i):
        return pltpu.make_async_copy(
            x_hbm.at[pl.ds(i * rows, rows), :], xs.at[z * chunks + i], local_sem.at[3 + i]
        )

    def give_rows(i, to_right):
        side = right if to_right else left
        sem = z * chunks + i if to_right else nz * chunks + i
        return remote(
            xs.at[z * chunks + i],
            xs.at[z * chunks + i],
            x_send.at[sem],
            x_recv.at[z * chunks + i],
            side,
        )

    def pass_rows(at, to_right):
        side = right if to_right else left
        return remote(xs.at[at], xs.at[at], x_send.at[at], x_recv.at[at], side)

    def pass_routes(source, to_right):
        side = right if to_right else left
        return remote(
            routes.at[source],
            routes.at[source],
            t_send.at[source if to_right else source + 1],
            t_recv.at[source],
            side,
        )

    seq = ql.shape[0]
    latent = keys.shape[0]
    turn = qr_hbm.shape[1] // uv.shape[0]
    mine_at = pl.ds(pl.multiple_of(ctx * seq, seq), seq)
    key_parts = (
        (lk_hbm, keys.at[:, mine_at]),
        (rk_hbm, ropes.at[0, pl.ds(0, turn), mine_at]),
        (rk_hbm, ropes.at[1, pl.ds(turn, turn), mine_at]),
    )

    def local_attention():
        pairs = key_parts + ((ql_hbm, ql), (qr_hbm, qr), (uv_hbm, uv))
        return [
            pltpu.make_async_copy(src, dst, a_local.at[n]) for n, (src, dst) in enumerate(pairs)
        ]

    def give_keys():
        return [
            remote(src, dst, a_send.at[n], a_recv.at[n], across)
            for n, (src, dst) in enumerate(key_parts)
        ]

    def put_attention():
        return pltpu.make_async_copy(attn, attn_hbm, a_local.at[6])

    def attend(head):
        span = keys.shape[1]
        value = uv.shape[2]
        pair = head // 2
        query = ctx * seq + lax.broadcasted_iota(jnp.int32, (seq, span), 0)
        visible = lax.broadcasted_iota(jnp.int32, (seq, span), 1) <= query
        query_lat = ql[:, pl.ds(pl.multiple_of(head * latent, latent), latent)]
        query_rot = qr[:, pl.ds(pl.multiple_of(pair * 2 * turn, 2 * turn), 2 * turn)]
        rotary = ropes[lax.rem(head, 2)]
        scores = (mm(query_lat, keys[...]) + mm(query_rot, rotary)) * score_scale
        masked = jnp.where(visible, scores, neg_large)
        top = jnp.max(masked, axis=1, keepdims=True)
        weights = jnp.where(visible, jnp.exp(masked - top), 0.0)
        whole = jnp.sum(weights, axis=1, keepdims=True)
        update = lax.dot_general(
            weights.astype(bf16), keys[...], (((1,), (1,)), ((), ())), preferred_element_type=f32
        )
        attn[:, pl.ds(pl.multiple_of(head * value, value), value)] = mm(
            (update / whole).astype(bf16), uv[head]
        ).astype(bf16)

    for i in range(chunks):
        own_rows(i).start()

    ropes[0, turn:, :] = jnp.zeros((turn, ropes.shape[2]), bf16)
    ropes[1, :turn, :] = jnp.zeros((turn, ropes.shape[2]), bf16)
    for expert in range(nz):
        line = jnp.zeros((1, routes.shape[3]), f32)
        for k in range(ids_ref.shape[0]):
            line = line + jnp.where(
                ids_ref[k : k + 1, :] == expert, scale_ref[k : k + 1, :], 0.0
            )
        routes[z, expert] = line

    @pl.when((z == 0) | (z == last))
    def _():
        pl.semaphore_wait(barrier, 3)

    @pl.when((z > 0) & (z < last))
    def _():
        pl.semaphore_wait(barrier, 4)

    @pl.when(z < last)
    def _():
        pass_routes(z, True).start()

    @pl.when(z > 0)
    def _():
        pass_routes(z, False).start()

    for i in range(half):
        own_rows(i).wait()

        @pl.when(z < last)
        def _():
            give_rows(i, True).start()

        @pl.when(z > 0)
        def _():
            give_rows(i, False).start()

    def give_rest(to_right):
        for i in range(half, chunks):
            give_rows(i, to_right).start()

    for k in range(2):
        own_weights(k).start()
    for i in range(half, chunks):
        own_rows(i).wait()

    @pl.when(z == 0)
    def _():
        give_rest(True)

    @pl.when(z == last)
    def _():
        give_rest(False)

    for copy in local_attention() + give_keys():
        copy.start()
    for k in range(2):
        give_weights(k).start()
    own_weights(2).start()
    give_weights(2).start()
    row_group = lax.broadcasted_iota(jnp.int32, (rows, 128), 0) // 8
    lane = lax.broadcasted_iota(jnp.int32, (rows, 128), 1)
    block = fh if width % fh == 0 else 128

    def spread(packed):
        tall = jnp.broadcast_to(packed[None], (groups, 8, 128)).reshape(rows, 128)
        return jnp.sum(jnp.where(lane == row_group, tall, 0.0), axis=1, keepdims=True)

    def weights_of(source, i):
        tokens = routes.shape[3]
        shape = (rows, tokens)
        wanted = lax.broadcasted_iota(jnp.int32, shape, 0) + i * rows
        hit = lax.broadcasted_iota(jnp.int32, shape, 1) == wanted
        line = jnp.broadcast_to(routes[source, z], shape)
        return jnp.sum(jnp.where(hit, line, 0.0), axis=1, keepdims=True)

    def exchange(at, slot, lane_at):
        return (
            remote(
                outgoing.at[slot, lane_at], theirs.at[at], p_send.at[at], p_recv.at[at], across
            ),
            remote(
                squares.at[slot, lane_at], squares_in.at[at], q_send.at[at], q_recv.at[at], across
            ),
        )

    def normalise(at, slot, lane_at):
        lines = pl.ds(lane_at * rows, rows)

        def columns(n, total):
            cols = pl.ds(pl.multiple_of(n * block, block), block)
            wide = xs[at, :, cols].astype(f32)
            scaled[lines, cols] = (wide * gain_ref[cols][None, :]).astype(bf16)
            square = wide * wide
            for m in range(block // 128):
                total = total + square[:, m * 128 : (m + 1) * 128]
            return total

        total = lax.fori_loop(0, width // block, columns, jnp.zeros((rows, 128), f32))
        column = jnp.sum(total, axis=1, keepdims=True)
        packed = jnp.where(lane == row_group, jnp.broadcast_to(column, (rows, 128)), 0.0)
        squares[slot, lane_at] = jnp.sum(packed.reshape(groups, 8, 128), axis=0)

    def project(t):
        slot = lax.rem(t, LAG + 1)
        places = [place(t, n) for n in range(2)]
        for n, (source, i, there) in enumerate(places):

            @pl.when(there)
            def _():
                normalise(source * chunks + i, slot, n)

        @pl.when(places[0][2] | places[1][2])
        def _():
            @pl.loop(0, 4)
            def _(k):
                part = jnp.dot(scaled[...], wgu[k], preferred_element_type=f32)
                mine[slot, k] = part
                for n in range(2):
                    outgoing[slot, n, k] = part[n * rows : (n + 1) * rows].astype(bf16)

        for n, (source, i, there) in enumerate(places):

            @pl.when(there)
            def _():
                for copy in exchange(source * chunks + i, slot, n):
                    copy.start()

    def activate(source, i, slot, lane_at):
        at = source * chunks + i
        lines = pl.ds(lane_at * rows, rows)
        for copy in exchange(at, slot, lane_at):
            copy.wait()
        square = spread(squares[slot, lane_at] + squares_in[at])
        scale = lax.rsqrt(square / total_width + norm_eps)
        weight = weights_of(source, i)

        @pl.loop(0, 2)
        def _(b):
            gate = (mine[slot, b, lines] + theirs[at, b].astype(f32)) * scale
            up = (mine[slot, b + 2, lines] + theirs[at, b + 2].astype(f32)) * scale
            hid = jax.nn.silu(gate) * up * weight
            scaled[lines, pl.ds(pl.multiple_of(b * fh, fh), fh)] = hid.astype(bf16)

    def expand(t):
        slot = lax.rem(t + LAG + 1, LAG + 1)
        places = [place(t, n) for n in range(2)]
        for n, (source, i, there) in enumerate(places):

            @pl.when(there)
            def _():
                activate(source, i, slot, n)

        @pl.when(places[0][2] | places[1][2])
        def _():
            @pl.loop(0, width // block)
            def _(b):
                cols = pl.ds(pl.multiple_of(b * block, block), block)
                part = jnp.dot(scaled[:, : 2 * fh], wd[:, cols], preferred_element_type=f32)
                for n, (source, i, there) in enumerate(places):

                    @pl.when(there)
                    def _():
                        con[source * chunks + i, :, cols] = part[
                            n * rows : (n + 1) * rows
                        ].astype(bf16)

    def arrival(k, from_left):
        near = z if from_left else last - z
        part = k // half
        late = part >= near
        source = jnp.where(late, part - near, near - 1 - part)
        i = lax.rem(k, half) + jnp.where(late, half, 0)
        there = (k >= 0) & (k < near * chunks)
        return source if from_left else last - source, i, there

    def place(t, lane_at):
        source, i, there = arrival(t, lane_at == 0)
        own_i = t - (spans - chunks)
        own = (own_i >= 0) & (own_i < chunks)
        own = own & ((z < last) if lane_at == 0 else (z == last))
        own = own & jnp.logical_not(there)
        return jnp.where(own, z, source), jnp.where(own, own_i, i), there | own

    def give_back(source, i, to_left, home=False):
        at = source * chunks + i
        to = at if to_left else at + chunks
        side = left if to_left else right
        lines = pl.ds(pl.multiple_of(i * rows, rows), rows)
        dst = (right_hbm if to_left else left_hbm).at[lines] if home else ret.at[to]
        return remote(con.at[at], dst, r_send.at[at], r_recv.at[to], side)

    def send_back(source, i, to_left):
        is_home = source == (z - 1 if to_left else z + 1)

        @pl.when(is_home)
        def _():
            give_back(source, i, to_left, True).start()

        @pl.when(jnp.logical_not(is_home))
        def _():
            give_back(source, i, to_left).start()

    def put_own(i):
        lines = pl.ds(pl.multiple_of(i * rows, rows), rows)
        return pltpu.make_async_copy(con.at[z * chunks + i], own_hbm.at[lines], o_sem.at[i])

    def await_back(source, i, to_left):
        at = source * chunks + i
        to = at if to_left else at + chunks
        remote(con.at[at], ret.at[to], r_send.at[at], r_recv.at[to], left).wait_recv()
        return to

    def add_back(source, i, tos):
        at = source * chunks + i

        @pl.loop(0, width // block)
        def _(n):
            cols = pl.ds(pl.multiple_of(n * block, block), block)
            value = con[at, :, cols].astype(f32)
            for to in tos:
                value = value + ret[to, :, cols].astype(f32)
            con[at, :, cols] = value.astype(bf16)

    def slot_step(t, carry):
        for to_right in (True, False):
            source, i, there = arrival(t, to_right)
            onward = (z < last) if to_right else (z > 0)
            near = z if to_right else last - z

            @pl.when(there)
            def _():
                at = source * chunks + i
                pass_rows(at, to_right).wait_recv()

                @pl.when(onward)
                def _():
                    pass_rows(at, to_right).start()

                @pl.when(i == 0)
                def _():
                    pass_routes(source, to_right).wait_recv()

                    @pl.when(onward)
                    def _():
                        pass_routes(source, to_right).start()

            @pl.when(onward & (near > 0) & (t == near * chunks - 1))
            def _():
                give_rest(to_right)

        @pl.when(t == 0)
        def _():
            for k in range(2):
                own_weights(k).wait()
                give_weights(k).wait()

        project(t)

        @pl.when(t == LAG)
        def _():
            own_weights(2).wait()
            give_weights(2).wait()

        heads = uv.shape[0]

        @pl.when(t == chunks)
        def _():
            for copy in local_attention():
                copy.wait()
            for copy in give_keys():
                copy.wait()

        @pl.when((t >= chunks) & (t < chunks + heads))
        def _():
            attend(t - chunks)

        @pl.when(t == chunks + heads)
        def _():
            put_attention().start()

        expand(t - LAG)

        own_i = t - LAG - (spans - chunks)

        @pl.when((own_i >= 0) & (own_i < chunks))
        def _():
            put_own(own_i).start()

        for to_left in (True, False):
            near = z if to_left else last - z
            source, i, there = arrival(t - LAG, to_left)

            @pl.when(there & (near == last))
            def _():
                send_back(source, i, to_left)

            k = t + half - (nz - near) * chunks
            source_back, i_back, there_back = arrival(k, to_left)

            @pl.when(there_back & (near < last))
            def _():
                to = await_back(source_back, i_back, to_left)
                add_back(source_back, i_back, [to])
                send_back(source_back, i_back, to_left)

        return carry

    lax.fori_loop(0, nz * chunks, slot_step, 0)

    for i in range(chunks):
        put_own(i).wait()

        @pl.when(z < last)
        def _():
            give_back(z, i, True, True).wait_recv()

        @pl.when(z > 0)
        def _():
            give_back(z, i, False, True).wait_recv()

    put_attention().wait()
    for i in range(chunks):

        @pl.when(z < last)
        def _():
            give_rows(i, True).wait_send()

        @pl.when(z > 0)
        def _():
            give_rows(i, False).wait_send()

    @pl.when(z < last)
    def _():
        pass_routes(z, True).wait_send()

    @pl.when(z > 0)
    def _():
        pass_routes(z, False).wait_send()

    def settle(t, carry):
        for to_right in (True, False):
            source, i, there = arrival(t, to_right)
            onward = (z < last) if to_right else (z > 0)

            @pl.when(there)
            def _():
                give_back(source, i, to_right).wait_send()

                @pl.when(onward)
                def _():
                    pass_rows(source * chunks + i, to_right).wait_send()

                @pl.when(onward & (i == 0))
                def _():
                    pass_routes(source, to_right).wait_send()

        return carry

    lax.fori_loop(0, spans, settle, 0)


def gather_kernel(last, attn_in, own_ref, right_ref, left_ref, attn_out, out_ref):
    z = lax.axis_index("ep") // 2
    attn_out[...] = attn_in[...]
    value = own_ref[...].astype(f32)
    value = value + jnp.where(z < last, right_ref[...].astype(f32), 0.0)
    value = value + jnp.where(z > 0, left_ref[...].astype(f32), 0.0)
    out_ref[...] = value.astype(bf16)


def expert_scratch(nz, rows, width, fh, seq, heads, latent, turn, value, tokens):
    jobs = nz * CHUNKS
    dma = pltpu.SemaphoreType.DMA
    return [
        pltpu.VMEM((seq, heads * latent), bf16),
        pltpu.VMEM((seq, heads * turn), bf16),
        pltpu.VMEM((latent, 2 * seq), bf16),
        pltpu.VMEM((2, 2 * turn, 2 * seq), bf16),
        pltpu.VMEM((heads, latent, value), bf16),
        pltpu.VMEM((seq, heads * value), bf16),
        pltpu.VMEM((jobs, rows, width), bf16),
        pltpu.VMEM((4, width, fh), bf16),
        pltpu.VMEM((2 * fh, width), bf16),
        pltpu.VMEM((jobs + CHUNKS, rows, width), bf16),
        pltpu.VMEM((jobs, rows, width), bf16),
        pltpu.VMEM((jobs, 4, rows, fh), bf16),
        pltpu.VMEM((LAG + 1, 4, 2 * rows, fh), f32),
        pltpu.VMEM((LAG + 1, 2, 4, rows, fh), bf16),
        pltpu.VMEM((2 * rows, width), bf16),
        pltpu.VMEM((LAG + 1, 2, 8, 128), f32),
        pltpu.VMEM((jobs, 8, 128), f32),
        pltpu.VMEM((nz, nz, 1, tokens), f32),
        dma((7,)),
        dma((3,)),
        dma((3,)),
        dma((3 + CHUNKS,)),
        dma((3,)),
        dma((3,)),
        dma((jobs + CHUNKS,)),
        dma((jobs,)),
        dma((jobs,)),
        dma((jobs + CHUNKS,)),
        dma((jobs,)),
        dma((jobs,)),
        dma((jobs,)),
        dma((jobs,)),
        dma((nz + 1,)),
        dma((nz,)),
        dma((CHUNKS,)),
    ]


def scratch_bytes(shapes):
    total = 0
    for s in shapes:
        if s.memory_space == pltpu.VMEM:
            n = jnp.dtype(s.dtype).itemsize
            for d in s.shape:
                n *= d
            total += n
    return total


def sizes(latent_keys, rope_keys, w_uv, moe_tokens, w_gate):
    heads, latent, value = w_uv.shape
    tokens, width = moe_tokens.shape
    return dict(
        nz=lax.axis_size("ep") // 2,
        rows=tokens // CHUNKS,
        width=width,
        fh=w_gate.shape[2],
        seq=latent_keys.shape[1],
        heads=heads,
        latent=latent,
        turn=rope_keys.shape[0],
        value=value,
        tokens=tokens,
    )


def fits(n, w_gate):
    n_ep = lax.axis_size("ep")
    if lax.axis_size("ctx") != 2 or n_ep % 2 or n["nz"] < 2 or w_gate.shape[0] != 1:
        return False
    if n["tokens"] % (16 * CHUNKS) or n["rows"] > 1024 or n["heads"] > (n["nz"] - 1) * CHUNKS:
        return False
    lanes = ("width", "fh", "seq", "latent", "value", "tokens")
    if any(n[name] % 128 for name in lanes) or n["turn"] != 64 or n["heads"] % 2:
        return False
    return scratch_bytes(expert_scratch(**n)) < VMEM_BYTES - 2**20


def fused(n, attention_in, moe_in):
    moe_tokens, norm_gain, expert_ids, route_scale, w_gate, w_up, w_down = moe_in
    anywhere = pl.BlockSpec(memory_space=pl.ANY)
    whole = pl.BlockSpec(memory_space=pltpu.VMEM)
    total = n["width"] * lax.axis_size("ctx")
    attn_shape = jax.ShapeDtypeStruct((n["seq"], n["heads"] * n["value"]), bf16)
    rows_shape = jax.ShapeDtypeStruct((n["tokens"], n["width"]), bf16)
    parts = pl.pallas_call(
        functools.partial(expert_kernel, n["nz"], CHUNKS, total),
        out_shape=(attn_shape, rows_shape, rows_shape, rows_shape),
        in_specs=[anywhere] * 9 + [whole] * 3,
        out_specs=(anywhere,) * 4,
        scratch_shapes=expert_scratch(**n),
        compiler_params=pltpu.CompilerParams(
            collective_id=0, has_side_effects=True, vmem_limit_bytes=VMEM_BYTES
        ),
    )(*attention_in, moe_tokens, w_gate, w_up, w_down, norm_gain, expert_ids.T, route_scale.T)
    steps = STEPS if n["seq"] % (16 * STEPS) == 0 and n["tokens"] % (16 * STEPS) == 0 else 1
    attn_block = pl.BlockSpec((n["seq"] // steps, attn_shape.shape[1]), lambda i: (i, 0))
    rows_block = pl.BlockSpec((n["tokens"] // steps, n["width"]), lambda i: (i, 0))
    return pl.pallas_call(
        functools.partial(gather_kernel, n["nz"] - 1),
        grid=(steps,),
        out_shape=(attn_shape, rows_shape),
        in_specs=[attn_block] + [rows_block] * 3,
        out_specs=(attn_block, rows_block),
    )(*parts)


def body(
    q_latent,
    q_rope,
    latent_keys,
    rope_keys,
    w_uv,
    moe_tokens,
    norm_gain,
    expert_ids,
    route_scale,
    w_gate,
    w_up,
    w_down,
):
    n = sizes(latent_keys, rope_keys, w_uv, moe_tokens, w_gate)
    if not fits(n, w_gate):
        return hop_body(
            q_latent,
            q_rope,
            latent_keys,
            rope_keys,
            w_uv,
            moe_tokens,
            norm_gain,
            expert_ids,
            route_scale,
            w_gate,
            w_up,
            w_down,
        )
    attention_in = (q_latent, q_rope, latent_keys, rope_keys, w_uv)
    moe_in = (moe_tokens, norm_gain, expert_ids, route_scale, w_gate, w_up, w_down)
    return fused(n, attention_in, moe_in)


def solution(mesh):
    return jax.shard_map(
        body,
        mesh=mesh,
        in_specs=(
            P(("group", "ctx"), "ep"),
            P(("group", "ctx"), "ep"),
            P("group", "ctx"),
            P("group", "ctx"),
            P("ep", None, None),
            P(("group", "ep"), "ctx"),
            P("ctx"),
            P(("group", "ep"), None),
            P(("group", "ep"), None),
            P("ep", "ctx", None),
            P("ep", "ctx", None),
            P("ep", None, "ctx"),
        ),
        out_specs=(P(("group", "ctx"), "ep"), P(("group", "ep"), "ctx")),
        check_vma=False,
    )
```

```python
import functools
import jax
import jax.numpy as jnp
from jax import lax
from jax.experimental import pallas as pl
from jax.experimental.pallas import tpu as pltpu
from jax.sharding import PartitionSpec as P

score_scale = 192.0 ** (-0.5)
norm_eps = 1e-06
neg_large = -1e30
PIECES = 2
CHUNKS = 4
LAG = 2
VMEM_BYTES = 67043328
f32 = jnp.float32
bf16 = jnp.bfloat16


def mm(a, b):
    return jnp.dot(a, b, preferred_element_type=f32)


def mm_t(a, b):
    return lax.dot_general(a, b, (((0,), (0,)), ((), ())), preferred_element_type=f32)


def swap_ctx(x):
    return lax.ppermute(x, "ctx", [(0, 1), (1, 0)])


def gather_keys(mine, ctx):
    if lax.axis_size("ctx") != 2:
        return lax.all_gather(mine, "ctx", axis=1, tiled=True)
    other = swap_ctx(mine)
    first = ctx == 0
    return jnp.concatenate(
        [jnp.where(first, mine, other), jnp.where(first, other, mine)], axis=1
    )


def sum_ctx(x):
    if lax.axis_size("ctx") != 2:
        return lax.psum(x, "ctx")
    return x + swap_ctx(x)


def attention(q_latent, q_rope, latent_keys, rope_keys, w_uv):
    seq_rows = q_latent.shape[0]
    head_count = w_uv.shape[0]
    latent_dim = latent_keys.shape[0]
    rope_dim = rope_keys.shape[0]
    query_lat = (
        q_latent.reshape(seq_rows, head_count, latent_dim)
        .transpose(1, 0, 2)
        .reshape(head_count * seq_rows, latent_dim)
    )
    query_rot = (
        q_rope.reshape(seq_rows, head_count, rope_dim)
        .transpose(1, 0, 2)
        .reshape(head_count * seq_rows, rope_dim)
    )
    ctx = lax.axis_index("ctx")
    query_pos = ctx * seq_rows + jnp.tile(jnp.arange(seq_rows, dtype=jnp.int32), head_count)
    mine = jnp.concatenate([latent_keys, rope_keys], axis=0)
    keys = gather_keys(mine, ctx)
    lat, rope = keys[:latent_dim], keys[latent_dim:]
    scores = (mm(query_lat, lat) + mm(query_rot, rope)) * score_scale
    key_pos = jnp.arange(lat.shape[1], dtype=jnp.int32)
    visible = key_pos[None, :] <= query_pos[:, None]
    masked = jnp.where(visible, scores, neg_large)
    top = jnp.max(masked, axis=1, keepdims=True)
    weights = jnp.where(visible, jnp.exp(masked - top), 0.0)
    total = jnp.sum(weights, axis=1, keepdims=True)
    update = lax.dot_general(
        weights.astype(bf16), lat, (((1,), (1,)), ((), ())), preferred_element_type=f32
    )
    context = (update / total).astype(bf16).reshape(head_count, seq_rows, latent_dim)
    heads = jnp.einsum("hsl,hlv->shv", context, w_uv, preferred_element_type=f32)
    return heads.reshape(seq_rows, head_count * w_uv.shape[2]).astype(bf16)


def ranks(key):
    n = key.shape[0]
    at = jnp.arange(n, dtype=jnp.int32)
    ahead = (key[None, :] > key[:, None]) | (
        (key[None, :] == key[:, None]) & (at[None, :] < at[:, None])
    )
    return jnp.sum(ahead.astype(jnp.int32), axis=1)


def position(ids, to_right):
    return ranks(jnp.where(to_right, jnp.max(ids, axis=1), -jnp.min(ids, axis=1)))


def hop_body(
    q_latent,
    q_rope,
    latent_keys,
    rope_keys,
    w_uv,
    moe_tokens,
    norm_gain,
    expert_ids,
    route_scale,
    w_gate,
    w_up,
    w_down,
):
    n_ep = lax.axis_size("ep")
    nz = n_ep // 2
    rows, top_count = expert_ids.shape
    cap = min(rows, 3 * rows * top_count // (2 * nz))
    half = cap // 2
    width = moe_tokens.shape[1]
    ep = lax.axis_index("ep")
    z = ep // 2
    ctx = lax.axis_index("ctx")
    group = -(-128 // cap)
    bands = [
        (b, cap * b, min(rows, cap * (b + group)))
        for b in range(0, nz - 1, group)
        if cap * b < rows
    ]
    pieces = max(1, PIECES * width // 3584)

    def hop(x, pairs):
        return lax.ppermute(
            x, "ep", [(2 * a + c, 2 * b + c) for a, b in pairs for c in range(2)]
        )

    info = jnp.concatenate([expert_ids.astype(f32), route_scale], axis=1)
    infos = {0: info}
    for k in range(1, nz):
        infos[k] = hop(info, [(a, (a + k) % nz) for a in range(nz)])

    def partner(x):
        return lax.ppermute(x, "ep", [(i, i ^ 1) for i in range(n_ep)])

    wide = moe_tokens.astype(f32)
    local_sq = jnp.sum(wide * wide, axis=1)
    total_sq = sum_ctx(local_sq)
    scale_rows = lax.rsqrt(total_sq / (width * lax.axis_size("ctx")) + norm_eps)
    normed = (wide * scale_rows[:, None] * norm_gain[None, :]).astype(bf16)

    slots = jnp.arange(rows, dtype=jnp.int32)
    pos_right = position(expert_ids, True)
    pos_left = position(expert_ids, False)
    perm_right = (pos_right[None, :] == slots[:, None]).astype(bf16)
    perm_left = (pos_left[None, :] == slots[:, None]).astype(bf16)

    gates = [w_gate[0], partner(w_gate[0])]
    ups = [w_up[0], partner(w_up[0])]
    downs = [w_down[0], partner(w_down[0])]

    held = {}
    for to_right, perm in ((True, perm_right), (False, perm_left)):
        for b, lo, hi in bands:
            block = mm(perm[lo:hi], normed).astype(bf16)
            for k in range(1, nz):
                if to_right:
                    pairs = [(a, a + 1) for a in range(k - 1, nz - 1 - b)]
                else:
                    pairs = [(nz - 1 - a, nz - 2 - a) for a in range(k - 1, nz - 1 - b)]
                if not pairs:
                    break
                block = hop(block, pairs)
                held[to_right, k, b] = block

    def chunk_of(zz, j):
        m = min(zz, nz - 1 - zz)
        if j <= 2 * m:
            return (j % 2 == 1, (j + 1) // 2)
        return (zz > nz - 1 - zz, j - m)

    expert = z

    def picks(ids, scales):
        hits = jnp.any(ids == expert, axis=1)
        at = jnp.arange(rows, dtype=jnp.int32)
        before = hits[None, :] & (at[None, :] < at[:, None])
        slot = jnp.sum(before.astype(jnp.int32), axis=1)
        sel = hits[None, :] & (slot[None, :] == jnp.arange(cap, dtype=jnp.int32)[:, None])
        own = jnp.sum(jnp.where(ids == expert, scales, 0.0), axis=1)
        return sel.astype(bf16), own

    def hidden_of(rows_in, sel):
        parts = jnp.concatenate(
            [mm(rows_in, w) for w in (gates[0], gates[1], ups[0], ups[1])], axis=1
        )
        units = parts.shape[1] // 2

        def act(both):
            return (jax.nn.silu(both[:, :units]) * both[:, units:]).astype(bf16)

        if lax.axis_size("ctx") != 2:
            both = lax.psum_scatter(parts.astype(bf16), "ctx", scatter_dimension=0, tiled=True)
            hid = lax.all_gather(act(both.astype(f32)), "ctx", axis=0, tiled=True)
            return mm_t(sel, hid).astype(bf16)
        theirs = lax.dynamic_slice_in_dim(parts, (1 - ctx) * half, half, 0).astype(bf16)
        mine = lax.dynamic_slice_in_dim(parts, ctx * half, half, 0)
        hid = act(mine + swap_ctx(theirs).astype(f32))
        hid_other = swap_ctx(hid)
        sel_mine = lax.dynamic_slice_in_dim(sel, ctx * half, half, 0)
        sel_other = lax.dynamic_slice_in_dim(sel, (1 - ctx) * half, half, 0)
        return (mm_t(sel_mine, hid) + mm_t(sel_other, hid_other)).astype(bf16)

    fh = w_gate.shape[2]
    step = width // pieces

    def contribution(hid, scale, piece):
        cols = slice(piece * step, (piece + 1) * step)
        out = mm(hid[:, :fh], downs[0][:, cols]) + mm(hid[:, fh:], downs[1][:, cols])
        return out * scale[:, None]

    sel_own, scale_own = picks(expert_ids, route_scale)
    hid_own = hidden_of(mm(sel_own, normed).astype(bf16), sel_own)

    hids = {}
    for j in range(1, nz):
        kinds = [chunk_of(zz, j) for zz in range(nz)]
        distinct = sorted(set(kinds))

        def choose(get):
            value = None
            for kind in distinct:
                here = False
                for zz in range(nz):
                    if kinds[zz] == kind:
                        here = here | (z == zz)
                got = get(kind)
                if got is None:
                    continue
                value = got if value is None else jnp.where(here, got, value)
            return value

        def source_info(kind):
            to_right, k = kind
            return infos[k] if to_right else infos[nz - k]

        chosen = choose(source_info)
        from_left = choose(lambda kind: jnp.full((1,), kind[0], jnp.bool_))[0]
        ids = chosen[:, :top_count].astype(jnp.int32)
        sel, scale = picks(ids, chosen[:, top_count:])
        pos = position(ids, from_left)
        place = (pos[:, None] == slots[None, :]).astype(bf16)
        sel_at = mm(sel, place).astype(bf16)
        scale_at = jnp.sum(jnp.where(pos[:, None] == slots[None, :], scale[:, None], 0.0), axis=0)
        rows_in = None
        for b, lo, hi in bands:
            block = choose(lambda kind: held.get((kind[0], kind[1], b)))
            if block is None:
                continue
            part = mm(sel_at[:, lo:hi], block)
            rows_in = part if rows_in is None else rows_in + part
        hids[j] = (hidden_of(rows_in.astype(bf16), sel_at), scale_at, kinds)

    def chunk_for(to_right, k):
        hid = scale = None
        for j in range(1, nz):
            zs = [zz for zz in range(nz) if hids[j][2][zz] == (to_right, k)]
            if not zs:
                continue
            here = False
            for zz in zs:
                here = here | (z == zz)
            if hid is None:
                hid = jnp.where(here, hids[j][0], 0)
                scale = jnp.where(here, hids[j][1], 0)
            else:
                hid = jnp.where(here, hids[j][0], hid)
                scale = jnp.where(here, hids[j][1], scale)
        return hid, scale

    returned = {}
    for k in range(nz - 1, 0, -1):
        for to_right in (True, False):
            hid, scale = chunk_for(to_right, k)
            for piece in range(pieces):
                acc = contribution(hid, scale, piece)
                for b, lo, hi in bands:
                    value = acc[lo:hi]
                    before = returned.get((to_right, piece, b))
                    if before is not None:
                        value = value + before.astype(f32)
                    pairs = [(a + 1, a) for a in range(k - 1, nz - 1 - b)]
                    if not to_right:
                        pairs = [(nz - 1 - p, nz - 1 - q) for p, q in pairs]
                    if pairs:
                        returned[to_right, piece, b] = hop(value.astype(bf16), pairs)

    outs = []
    for piece in range(pieces):
        acc = contribution(hid_own, scale_own, piece)
        for to_right, perm in ((True, perm_right), (False, perm_left)):
            for b, lo, hi in bands:
                got = returned.get((to_right, piece, b))
                if got is not None:
                    acc = acc + mm_t(perm[lo:hi], got)
        outs.append(acc.astype(bf16))
    moe_out = jnp.concatenate(outs, axis=1)
    attn_out = attention(q_latent, q_rope, latent_keys, rope_keys, w_uv)
    return (attn_out, moe_out)


def expert_kernel(
    nz,
    chunks,
    total_width,
    ql_hbm,
    qr_hbm,
    lk_hbm,
    rk_hbm,
    uv_hbm,
    x_hbm,
    wg_hbm,
    wu_hbm,
    wd_hbm,
    gain_hbm,
    ids_hbm,
    scale_hbm,
    attn_hbm,
    own_hbm,
    right_hbm,
    left_hbm,
    gain_ref,
    ids_ref,
    scale_ref,
    ql,
    qr,
    keys,
    ropes,
    uv,
    attn,
    xs,
    wgu,
    wd,
    ret,
    con,
    theirs,
    mine,
    outgoing,
    scaled,
    squares,
    squares_in,
    routes,
    a_local,
    a_send,
    a_recv,
    local_sem,
    w_send,
    w_recv,
    x_send,
    x_recv,
    r_send,
    r_recv,
    p_send,
    p_recv,
    q_send,
    q_recv,
    t_send,
    t_recv,
    o_sem,
    s_sem,
):
    ep = lax.axis_index("ep")
    z = ep // 2
    core = ep % 2
    ctx = lax.axis_index("ctx")
    rows, width = xs.shape[1], xs.shape[2]
    fh = wgu.shape[2]
    groups = rows // 8
    last = nz - 1
    spans = last * chunks
    half = chunks // 2
    left, right = {"ep": ep - 2}, {"ep": ep + 2}
    across = {"ctx": 1 - ctx}
    beside = {"ep": 2 * z + 1 - core}

    def remote(src, dst, send, recv, device):
        return pltpu.make_async_remote_copy(
            src_ref=src,
            dst_ref=dst,
            send_sem=send,
            recv_sem=recv,
            device_id=device,
            device_id_type=pl.DeviceIdType.MESH,
        )

    barrier = pltpu.get_barrier_semaphore()
    for near, device in ((z > 0, left), (z < last, right)):

        @pl.when(near)
        def _():
            pl.semaphore_signal(
                barrier, inc=1, device_id=device, device_id_type=pl.DeviceIdType.MESH
            )

    for device in (across, beside):
        pl.semaphore_signal(
            barrier, inc=1, device_id=device, device_id_type=pl.DeviceIdType.MESH
        )

    def own_weights(k):
        if k == 0:
            return pltpu.make_async_copy(wg_hbm.at[0], wgu.at[0], local_sem.at[0])
        if k == 1:
            return pltpu.make_async_copy(wu_hbm.at[0], wgu.at[2], local_sem.at[1])
        return pltpu.make_async_copy(wd_hbm.at[0], wd.at[pl.ds(0, fh), :], local_sem.at[2])

    def give_weights(k):
        src = (wg_hbm, wu_hbm, wd_hbm)[k].at[0]
        dst = (wgu.at[1], wgu.at[3], wd.at[pl.ds(fh, fh), :])[k]
        return remote(src, dst, w_send.at[k], w_recv.at[k], beside)

    def own_rows(i):
        return pltpu.make_async_copy(
            x_hbm.at[pl.ds(i * rows, rows), :], xs.at[z * chunks + i], local_sem.at[3 + i]
        )

    def give_rows(i, to_right):
        side = right if to_right else left
        sem = z * chunks + i if to_right else nz * chunks + i
        return remote(
            xs.at[z * chunks + i],
            xs.at[z * chunks + i],
            x_send.at[sem],
            x_recv.at[z * chunks + i],
            side,
        )

    def pass_rows(at, to_right):
        side = right if to_right else left
        return remote(xs.at[at], xs.at[at], x_send.at[at], x_recv.at[at], side)

    def pass_routes(source, to_right):
        side = right if to_right else left
        return remote(
            routes.at[source],
            routes.at[source],
            t_send.at[source if to_right else source + 1],
            t_recv.at[source],
            side,
        )

    seq = ql.shape[0]
    latent = keys.shape[0]
    turn = qr_hbm.shape[1] // uv.shape[0]
    mine_at = pl.ds(pl.multiple_of(ctx * seq, seq), seq)
    key_parts = (
        (lk_hbm, keys.at[:, mine_at]),
        (rk_hbm, ropes.at[0, pl.ds(0, turn), mine_at]),
        (rk_hbm, ropes.at[1, pl.ds(turn, turn), mine_at]),
    )

    def local_attention():
        pairs = key_parts + ((ql_hbm, ql), (qr_hbm, qr), (uv_hbm, uv))
        return [
            pltpu.make_async_copy(src, dst, a_local.at[n]) for n, (src, dst) in enumerate(pairs)
        ]

    def give_keys():
        return [
            remote(src, dst, a_send.at[n], a_recv.at[n], across)
            for n, (src, dst) in enumerate(key_parts)
        ]

    def put_attention():
        return pltpu.make_async_copy(attn, attn_hbm, a_local.at[6])

    def attend(head):
        span = keys.shape[1]
        value = uv.shape[2]
        pair = head // 2
        query = ctx * seq + lax.broadcasted_iota(jnp.int32, (seq, span), 0)
        visible = lax.broadcasted_iota(jnp.int32, (seq, span), 1) <= query
        query_lat = ql[:, pl.ds(pl.multiple_of(head * latent, latent), latent)]
        query_rot = qr[:, pl.ds(pl.multiple_of(pair * 2 * turn, 2 * turn), 2 * turn)]
        rotary = ropes[lax.rem(head, 2)]
        scores = (mm(query_lat, keys[...]) + mm(query_rot, rotary)) * score_scale
        masked = jnp.where(visible, scores, neg_large)
        top = jnp.max(masked, axis=1, keepdims=True)
        weights = jnp.where(visible, jnp.exp(masked - top), 0.0)
        whole = jnp.sum(weights, axis=1, keepdims=True)
        update = lax.dot_general(
            weights.astype(bf16), keys[...], (((1,), (1,)), ((), ())), preferred_element_type=f32
        )
        attn[:, pl.ds(pl.multiple_of(head * value, value), value)] = mm(
            (update / whole).astype(bf16), uv[head]
        ).astype(bf16)

    for i in range(chunks):
        own_rows(i).start()

    small = [
        pltpu.make_async_copy(src, dst, s_sem.at[n])
        for n, (src, dst) in enumerate(
            ((ids_hbm, ids_ref), (scale_hbm, scale_ref), (gain_hbm, gain_ref))
        )
    ]
    for copy in small:
        copy.start()
    ropes[0, turn:, :] = jnp.zeros((turn, ropes.shape[2]), bf16)
    ropes[1, :turn, :] = jnp.zeros((turn, ropes.shape[2]), bf16)
    for copy in small:
        copy.wait()
    for expert in range(nz):
        line = jnp.zeros((1, routes.shape[3]), f32)
        for k in range(ids_ref.shape[0]):
            line = line + jnp.where(
                ids_ref[k : k + 1, :] == expert, scale_ref[k : k + 1, :], 0.0
            )
        routes[z, expert] = line

    @pl.when((z == 0) | (z == last))
    def _():
        pl.semaphore_wait(barrier, 3)

    @pl.when((z > 0) & (z < last))
    def _():
        pl.semaphore_wait(barrier, 4)

    @pl.when(z < last)
    def _():
        pass_routes(z, True).start()

    @pl.when(z > 0)
    def _():
        pass_routes(z, False).start()

    for i in range(half):
        own_rows(i).wait()

        @pl.when(z < last)
        def _():
            give_rows(i, True).start()

        @pl.when(z > 0)
        def _():
            give_rows(i, False).start()

    def give_rest(to_right):
        for i in range(half, chunks):
            give_rows(i, to_right).start()

    for k in range(2):
        own_weights(k).start()
    for i in range(half, chunks):
        own_rows(i).wait()

    @pl.when(z == 0)
    def _():
        give_rest(True)

    @pl.when(z == last)
    def _():
        give_rest(False)

    for copy in local_attention() + give_keys():
        copy.start()
    for k in range(2):
        give_weights(k).start()
    own_weights(2).start()
    give_weights(2).start()
    row_group = lax.broadcasted_iota(jnp.int32, (rows, 128), 0) // 8
    lane = lax.broadcasted_iota(jnp.int32, (rows, 128), 1)
    block = fh if width % fh == 0 else 128

    def spread(packed):
        tall = jnp.broadcast_to(packed[None], (groups, 8, 128)).reshape(rows, 128)
        return jnp.sum(jnp.where(lane == row_group, tall, 0.0), axis=1, keepdims=True)

    def weights_of(source, i):
        tokens = routes.shape[3]
        shape = (rows, tokens)
        wanted = lax.broadcasted_iota(jnp.int32, shape, 0) + i * rows
        hit = lax.broadcasted_iota(jnp.int32, shape, 1) == wanted
        line = jnp.broadcast_to(routes[source, z], shape)
        return jnp.sum(jnp.where(hit, line, 0.0), axis=1, keepdims=True)

    def exchange(at, slot, lane_at):
        return (
            remote(
                outgoing.at[slot, lane_at], theirs.at[at], p_send.at[at], p_recv.at[at], across
            ),
            remote(
                squares.at[slot, lane_at], squares_in.at[at], q_send.at[at], q_recv.at[at], across
            ),
        )

    def normalise(at, slot, lane_at):
        lines = pl.ds(lane_at * rows, rows)

        def columns(n, total):
            cols = pl.ds(pl.multiple_of(n * block, block), block)
            wide = xs[at, :, cols].astype(f32)
            scaled[lines, cols] = (wide * gain_ref[cols][None, :]).astype(bf16)
            square = wide * wide
            for m in range(block // 128):
                total = total + square[:, m * 128 : (m + 1) * 128]
            return total

        total = lax.fori_loop(0, width // block, columns, jnp.zeros((rows, 128), f32))
        column = jnp.sum(total, axis=1, keepdims=True)
        packed = jnp.where(lane == row_group, jnp.broadcast_to(column, (rows, 128)), 0.0)
        squares[slot, lane_at] = jnp.sum(packed.reshape(groups, 8, 128), axis=0)

    def project(t):
        slot = lax.rem(t, LAG + 1)
        places = [place(t, n) for n in range(2)]
        for n, (source, i, there) in enumerate(places):

            @pl.when(there)
            def _():
                normalise(source * chunks + i, slot, n)

        @pl.when(places[0][2] | places[1][2])
        def _():
            @pl.loop(0, 4)
            def _(k):
                part = jnp.dot(scaled[...], wgu[k], preferred_element_type=f32)
                mine[slot, k] = part
                for n in range(2):
                    outgoing[slot, n, k] = part[n * rows : (n + 1) * rows].astype(bf16)

        for n, (source, i, there) in enumerate(places):

            @pl.when(there)
            def _():
                for copy in exchange(source * chunks + i, slot, n):
                    copy.start()

    def activate(source, i, slot, lane_at):
        at = source * chunks + i
        lines = pl.ds(lane_at * rows, rows)
        for copy in exchange(at, slot, lane_at):
            copy.wait()
        square = spread(squares[slot, lane_at] + squares_in[at])
        scale = lax.rsqrt(square / total_width + norm_eps)
        weight = weights_of(source, i)

        @pl.loop(0, 2)
        def _(b):
            gate = (mine[slot, b, lines] + theirs[at, b].astype(f32)) * scale
            up = (mine[slot, b + 2, lines] + theirs[at, b + 2].astype(f32)) * scale
            hid = jax.nn.silu(gate) * up * weight
            scaled[lines, pl.ds(pl.multiple_of(b * fh, fh), fh)] = hid.astype(bf16)

    def expand(t):
        slot = lax.rem(t + LAG + 1, LAG + 1)
        places = [place(t, n) for n in range(2)]
        for n, (source, i, there) in enumerate(places):

            @pl.when(there)
            def _():
                activate(source, i, slot, n)

        @pl.when(places[0][2] | places[1][2])
        def _():
            @pl.loop(0, width // block)
            def _(b):
                cols = pl.ds(pl.multiple_of(b * block, block), block)
                part = jnp.dot(scaled[:, : 2 * fh], wd[:, cols], preferred_element_type=f32)
                for n, (source, i, there) in enumerate(places):

                    @pl.when(there)
                    def _():
                        con[source * chunks + i, :, cols] = part[
                            n * rows : (n + 1) * rows
                        ].astype(bf16)

    def arrival(k, from_left):
        near = z if from_left else last - z
        part = k // half
        late = part >= near
        source = jnp.where(late, part - near, near - 1 - part)
        i = lax.rem(k, half) + jnp.where(late, half, 0)
        there = (k >= 0) & (k < near * chunks)
        return source if from_left else last - source, i, there

    def place(t, lane_at):
        source, i, there = arrival(t, lane_at == 0)
        own_i = t - (spans - chunks)
        own = (own_i >= 0) & (own_i < chunks)
        own = own & ((z < last) if lane_at == 0 else (z == last))
        own = own & jnp.logical_not(there)
        return jnp.where(own, z, source), jnp.where(own, own_i, i), there | own

    def give_back(source, i, to_left, home=False):
        at = source * chunks + i
        to = at if to_left else at + chunks
        side = left if to_left else right
        dst = (right_hbm if to_left else left_hbm) if home else ret.at[to]
        return remote(con.at[at], dst, r_send.at[at], r_recv.at[to], side)

    def send_back(source, i, to_left):
        is_home = (source == (z - 1 if to_left else z + 1)) & (i == chunks - 1)

        @pl.when(is_home)
        def _():
            give_back(source, i, to_left, True).start()

        @pl.when(jnp.logical_not(is_home))
        def _():
            give_back(source, i, to_left).start()

    def put_own(i):
        lines = pl.ds(pl.multiple_of(i * rows, rows), rows)
        return pltpu.make_async_copy(con.at[z * chunks + i], own_hbm.at[lines], o_sem.at[i])

    def await_back(source, i, to_left):
        at = source * chunks + i
        to = at if to_left else at + chunks
        remote(con.at[at], ret.at[to], r_send.at[at], r_recv.at[to], left).wait_recv()
        return to

    def add_back(source, i, tos):
        at = source * chunks + i

        @pl.loop(0, width // block)
        def _(n):
            cols = pl.ds(pl.multiple_of(n * block, block), block)
            value = con[at, :, cols].astype(f32)
            for to in tos:
                value = value + ret[to, :, cols].astype(f32)
            con[at, :, cols] = value.astype(bf16)

    def slot_step(t, carry):
        for to_right in (True, False):
            source, i, there = arrival(t, to_right)
            onward = (z < last) if to_right else (z > 0)
            near = z if to_right else last - z

            @pl.when(there)
            def _():
                at = source * chunks + i
                pass_rows(at, to_right).wait_recv()

                @pl.when(onward)
                def _():
                    pass_rows(at, to_right).start()

                @pl.when(i == 0)
                def _():
                    pass_routes(source, to_right).wait_recv()

                    @pl.when(onward)
                    def _():
                        pass_routes(source, to_right).start()

            @pl.when(onward & (near > 0) & (t == near * chunks - 1))
            def _():
                give_rest(to_right)

        @pl.when(t == 0)
        def _():
            for k in range(2):
                own_weights(k).wait()
                give_weights(k).wait()

        project(t)

        @pl.when(t == LAG)
        def _():
            own_weights(2).wait()
            give_weights(2).wait()

        heads = uv.shape[0]

        @pl.when(t == chunks)
        def _():
            for copy in local_attention():
                copy.wait()
            for copy in give_keys():
                copy.wait()

        @pl.when((t >= chunks) & (t < chunks + heads))
        def _():
            attend(t - chunks)

        @pl.when(t == chunks + heads)
        def _():
            put_attention().start()

        expand(t - LAG)

        @pl.when(t - LAG == spans - 1)
        def _():
            put_own(chunks - 1).start()

        for to_left in (True, False):
            near = z if to_left else last - z
            source, i, there = arrival(t - LAG, to_left)

            @pl.when(there & (near == last))
            def _():
                send_back(source, i, to_left)

            k = t + half - (nz - near) * chunks
            source_back, i_back, there_back = arrival(k, to_left)

            @pl.when(there_back & (near < last))
            def _():
                to = await_back(source_back, i_back, to_left)
                add_back(source_back, i_back, [to])
                send_back(source_back, i_back, to_left)

        return carry

    lax.fori_loop(0, nz * chunks, slot_step, 0)

    for where, sides in (
        (z == 0, (True,)),
        (z == last, (False,)),
        ((z > 0) & (z < last), (True, False)),
    ):

        @pl.when(where)
        def _():
            @pl.loop(0, chunks - 1)
            def _(i):
                add_back(z, i, [await_back(z, i, to_left) for to_left in sides])
                put_own(i).start()

    put_attention().wait()
    for i in range(chunks):

        @pl.when(z < last)
        def _():
            give_rows(i, True).wait_send()

        @pl.when(z > 0)
        def _():
            give_rows(i, False).wait_send()

    @pl.when(z < last)
    def _():
        pass_routes(z, True).wait_send()

    @pl.when(z > 0)
    def _():
        pass_routes(z, False).wait_send()

    def settle(t, carry):
        for to_right in (True, False):
            source, i, there = arrival(t, to_right)
            onward = (z < last) if to_right else (z > 0)

            @pl.when(there)
            def _():
                give_back(source, i, to_right).wait_send()

                @pl.when(onward)
                def _():
                    pass_rows(source * chunks + i, to_right).wait_send()

                @pl.when(onward & (i == 0))
                def _():
                    pass_routes(source, to_right).wait_send()

        return carry

    lax.fori_loop(0, spans, settle, 0)

    for i in range(chunks):
        put_own(i).wait()

    @pl.when(z < last)
    def _():
        give_back(z, chunks - 1, True, True).wait_recv()

    @pl.when(z > 0)
    def _():
        give_back(z, chunks - 1, False, True).wait_recv()


def gather_kernel(
    last,
    chunks,
    attn_in,
    own_in,
    right_in,
    left_in,
    attn_out,
    out_hbm,
    attn,
    own,
    right,
    left,
    sem_in,
    sem_out,
):
    z = lax.axis_index("ep") // 2
    rows, width = right.shape

    def take(i):
        return pltpu.make_async_copy(own_in.at[pl.ds(i * rows, rows)], own.at[i], sem_in.at[i])

    def put(i):
        return pltpu.make_async_copy(own.at[i], out_hbm.at[pl.ds(i * rows, rows)], sem_out.at[i])

    final = chunks - 1
    take_right = pltpu.make_async_copy(right_in, right, sem_in.at[chunks])
    take_left = pltpu.make_async_copy(left_in, left, sem_in.at[chunks + 1])
    take_attn = pltpu.make_async_copy(attn_in, attn, sem_in.at[chunks + 2])
    put_attn = pltpu.make_async_copy(attn, attn_out, sem_out.at[chunks])
    take(final).start()
    take_right.start()
    take_left.start()
    take_attn.start()
    for i in range(final):
        take(i).start()
    take(final).wait()
    take_right.wait()
    take_left.wait()
    block = 512 if width % 512 == 0 else 128

    @pl.loop(0, width // block)
    def _(n):
        cols = pl.ds(pl.multiple_of(n * block, block), block)
        value = own[final, :, cols].astype(f32)
        value = value + jnp.where(z < last, right[:, cols].astype(f32), 0.0)
        value = value + jnp.where(z > 0, left[:, cols].astype(f32), 0.0)
        own[final, :, cols] = value.astype(bf16)

    put(final).start()
    take_attn.wait()
    put_attn.start()
    for i in range(final):
        take(i).wait()
        put(i).start()
    put_attn.wait()
    for i in range(chunks):
        put(i).wait()


def expert_scratch(nz, rows, width, fh, seq, heads, latent, turn, value, tokens, top):
    jobs = nz * CHUNKS
    dma = pltpu.SemaphoreType.DMA
    return [
        pltpu.VMEM((width,), f32),
        pltpu.VMEM((top, tokens), jnp.int32),
        pltpu.VMEM((top, tokens), f32),
        pltpu.VMEM((seq, heads * latent), bf16),
        pltpu.VMEM((seq, heads * turn), bf16),
        pltpu.VMEM((latent, 2 * seq), bf16),
        pltpu.VMEM((2, 2 * turn, 2 * seq), bf16),
        pltpu.VMEM((heads, latent, value), bf16),
        pltpu.VMEM((seq, heads * value), bf16),
        pltpu.VMEM((jobs, rows, width), bf16),
        pltpu.VMEM((4, width, fh), bf16),
        pltpu.VMEM((2 * fh, width), bf16),
        pltpu.VMEM((jobs + CHUNKS, rows, width), bf16),
        pltpu.VMEM((jobs, rows, width), bf16),
        pltpu.VMEM((jobs, 4, rows, fh), bf16),
        pltpu.VMEM((LAG + 1, 4, 2 * rows, fh), f32),
        pltpu.VMEM((LAG + 1, 2, 4, rows, fh), bf16),
        pltpu.VMEM((2 * rows, width), bf16),
        pltpu.VMEM((LAG + 1, 2, 8, 128), f32),
        pltpu.VMEM((jobs, 8, 128), f32),
        pltpu.VMEM((nz, nz, 1, tokens), f32),
        dma((7,)),
        dma((3,)),
        dma((3,)),
        dma((3 + CHUNKS,)),
        dma((3,)),
        dma((3,)),
        dma((jobs + CHUNKS,)),
        dma((jobs,)),
        dma((jobs,)),
        dma((jobs + CHUNKS,)),
        dma((jobs,)),
        dma((jobs,)),
        dma((jobs,)),
        dma((jobs,)),
        dma((nz + 1,)),
        dma((nz,)),
        dma((CHUNKS,)),
        dma((3,)),
    ]


def scratch_bytes(shapes):
    total = 0
    for s in shapes:
        if s.memory_space == pltpu.VMEM:
            n = jnp.dtype(s.dtype).itemsize
            for d in s.shape:
                n *= d
            total += n
    return total


def sizes(latent_keys, rope_keys, w_uv, moe_tokens, expert_ids, w_gate):
    heads, latent, value = w_uv.shape
    tokens, width = moe_tokens.shape
    return dict(
        nz=lax.axis_size("ep") // 2,
        rows=tokens // CHUNKS,
        width=width,
        fh=w_gate.shape[2],
        seq=latent_keys.shape[1],
        heads=heads,
        latent=latent,
        turn=rope_keys.shape[0],
        value=value,
        tokens=tokens,
        top=expert_ids.shape[1],
    )


def fits(n, w_gate):
    n_ep = lax.axis_size("ep")
    if lax.axis_size("ctx") != 2 or n_ep % 2 or n["nz"] < 2 or w_gate.shape[0] != 1:
        return False
    if n["tokens"] % (16 * CHUNKS) or n["rows"] > 1024 or n["heads"] > (n["nz"] - 1) * CHUNKS:
        return False
    lanes = ("width", "fh", "seq", "latent", "value", "tokens")
    if any(n[name] % 128 for name in lanes) or n["turn"] != 64 or n["heads"] % 2:
        return False
    return scratch_bytes(expert_scratch(**n)) < VMEM_BYTES - 2**20


def fused(n, attention_in, moe_in):
    moe_tokens, norm_gain, expert_ids, route_scale, w_gate, w_up, w_down = moe_in
    anywhere = pl.BlockSpec(memory_space=pl.ANY)
    total = n["width"] * lax.axis_size("ctx")
    attn_shape = jax.ShapeDtypeStruct((n["seq"], n["heads"] * n["value"]), bf16)
    rows_shape = jax.ShapeDtypeStruct((n["tokens"], n["width"]), bf16)
    last_shape = jax.ShapeDtypeStruct((n["rows"], n["width"]), bf16)
    parts = pl.pallas_call(
        functools.partial(expert_kernel, n["nz"], CHUNKS, total),
        out_shape=(attn_shape, rows_shape, last_shape, last_shape),
        in_specs=[anywhere] * 12,
        out_specs=(anywhere,) * 4,
        scratch_shapes=expert_scratch(**n),
        compiler_params=pltpu.CompilerParams(
            collective_id=0, has_side_effects=True, vmem_limit_bytes=VMEM_BYTES
        ),
    )(*attention_in, moe_tokens, w_gate, w_up, w_down, norm_gain, expert_ids.T, route_scale.T)
    dma = pltpu.SemaphoreType.DMA
    return pl.pallas_call(
        functools.partial(gather_kernel, n["nz"] - 1, CHUNKS),
        out_shape=(attn_shape, rows_shape),
        in_specs=[anywhere] * 4,
        out_specs=(anywhere, anywhere),
        scratch_shapes=[
            pltpu.VMEM(attn_shape.shape, bf16),
            pltpu.VMEM((CHUNKS, n["rows"], n["width"]), bf16),
            pltpu.VMEM(last_shape.shape, bf16),
            pltpu.VMEM(last_shape.shape, bf16),
            dma((CHUNKS + 3,)),
            dma((CHUNKS + 1,)),
        ],
        compiler_params=pltpu.CompilerParams(vmem_limit_bytes=VMEM_BYTES),
    )(*parts)


def body(
    q_latent,
    q_rope,
    latent_keys,
    rope_keys,
    w_uv,
    moe_tokens,
    norm_gain,
    expert_ids,
    route_scale,
    w_gate,
    w_up,
    w_down,
):
    n = sizes(latent_keys, rope_keys, w_uv, moe_tokens, expert_ids, w_gate)
    if not fits(n, w_gate):
        return hop_body(
            q_latent,
            q_rope,
            latent_keys,
            rope_keys,
            w_uv,
            moe_tokens,
            norm_gain,
            expert_ids,
            route_scale,
            w_gate,
            w_up,
            w_down,
        )
    attention_in = (q_latent, q_rope, latent_keys, rope_keys, w_uv)
    moe_in = (moe_tokens, norm_gain, expert_ids, route_scale, w_gate, w_up, w_down)
    return fused(n, attention_in, moe_in)


def solution(mesh):
    return jax.shard_map(
        body,
        mesh=mesh,
        in_specs=(
            P(("group", "ctx"), "ep"),
            P(("group", "ctx"), "ep"),
            P("group", "ctx"),
            P("group", "ctx"),
            P("ep", None, None),
            P(("group", "ep"), "ctx"),
            P("ctx"),
            P(("group", "ep"), None),
            P(("group", "ep"), None),
            P("ep", "ctx", None),
            P("ep", "ctx", None),
            P("ep", None, "ctx"),
        ),
        out_specs=(P(("group", "ctx"), "ep"), P(("group", "ep"), "ctx")),
        check_vma=False,
    )
```

```python
import functools
import jax
import jax.numpy as jnp
from jax import lax
from jax.experimental import pallas as pl
from jax.experimental.pallas import tpu as pltpu
from jax.sharding import PartitionSpec as P

score_scale = 192.0 ** (-0.5)
norm_eps = 1e-06
neg_large = -1e30
PIECES = 2
CHUNKS = 4
LAG = 2
VMEM_BYTES = 67043328
f32 = jnp.float32
bf16 = jnp.bfloat16


def mm(a, b):
    return jnp.dot(a, b, preferred_element_type=f32)


def mm_t(a, b):
    return lax.dot_general(a, b, (((0,), (0,)), ((), ())), preferred_element_type=f32)


def swap_ctx(x):
    return lax.ppermute(x, "ctx", [(0, 1), (1, 0)])


def gather_keys(mine, ctx):
    if lax.axis_size("ctx") != 2:
        return lax.all_gather(mine, "ctx", axis=1, tiled=True)
    other = swap_ctx(mine)
    first = ctx == 0
    return jnp.concatenate(
        [jnp.where(first, mine, other), jnp.where(first, other, mine)], axis=1
    )


def sum_ctx(x):
    if lax.axis_size("ctx") != 2:
        return lax.psum(x, "ctx")
    return x + swap_ctx(x)


def attention(q_latent, q_rope, latent_keys, rope_keys, w_uv):
    seq_rows = q_latent.shape[0]
    head_count = w_uv.shape[0]
    latent_dim = latent_keys.shape[0]
    rope_dim = rope_keys.shape[0]
    query_lat = (
        q_latent.reshape(seq_rows, head_count, latent_dim)
        .transpose(1, 0, 2)
        .reshape(head_count * seq_rows, latent_dim)
    )
    query_rot = (
        q_rope.reshape(seq_rows, head_count, rope_dim)
        .transpose(1, 0, 2)
        .reshape(head_count * seq_rows, rope_dim)
    )
    ctx = lax.axis_index("ctx")
    query_pos = ctx * seq_rows + jnp.tile(jnp.arange(seq_rows, dtype=jnp.int32), head_count)
    mine = jnp.concatenate([latent_keys, rope_keys], axis=0)
    keys = gather_keys(mine, ctx)
    lat, rope = keys[:latent_dim], keys[latent_dim:]
    scores = (mm(query_lat, lat) + mm(query_rot, rope)) * score_scale
    key_pos = jnp.arange(lat.shape[1], dtype=jnp.int32)
    visible = key_pos[None, :] <= query_pos[:, None]
    masked = jnp.where(visible, scores, neg_large)
    top = jnp.max(masked, axis=1, keepdims=True)
    weights = jnp.where(visible, jnp.exp(masked - top), 0.0)
    total = jnp.sum(weights, axis=1, keepdims=True)
    update = lax.dot_general(
        weights.astype(bf16), lat, (((1,), (1,)), ((), ())), preferred_element_type=f32
    )
    context = (update / total).astype(bf16).reshape(head_count, seq_rows, latent_dim)
    heads = jnp.einsum("hsl,hlv->shv", context, w_uv, preferred_element_type=f32)
    return heads.reshape(seq_rows, head_count * w_uv.shape[2]).astype(bf16)


def ranks(key):
    n = key.shape[0]
    at = jnp.arange(n, dtype=jnp.int32)
    ahead = (key[None, :] > key[:, None]) | (
        (key[None, :] == key[:, None]) & (at[None, :] < at[:, None])
    )
    return jnp.sum(ahead.astype(jnp.int32), axis=1)


def position(ids, to_right):
    return ranks(jnp.where(to_right, jnp.max(ids, axis=1), -jnp.min(ids, axis=1)))


def hop_body(
    q_latent,
    q_rope,
    latent_keys,
    rope_keys,
    w_uv,
    moe_tokens,
    norm_gain,
    expert_ids,
    route_scale,
    w_gate,
    w_up,
    w_down,
):
    n_ep = lax.axis_size("ep")
    nz = n_ep // 2
    rows, top_count = expert_ids.shape
    cap = min(rows, 3 * rows * top_count // (2 * nz))
    half = cap // 2
    width = moe_tokens.shape[1]
    ep = lax.axis_index("ep")
    z = ep // 2
    ctx = lax.axis_index("ctx")
    group = -(-128 // cap)
    bands = [
        (b, cap * b, min(rows, cap * (b + group)))
        for b in range(0, nz - 1, group)
        if cap * b < rows
    ]
    pieces = max(1, PIECES * width // 3584)

    def hop(x, pairs):
        return lax.ppermute(
            x, "ep", [(2 * a + c, 2 * b + c) for a, b in pairs for c in range(2)]
        )

    info = jnp.concatenate([expert_ids.astype(f32), route_scale], axis=1)
    infos = {0: info}
    for k in range(1, nz):
        infos[k] = hop(info, [(a, (a + k) % nz) for a in range(nz)])

    def partner(x):
        return lax.ppermute(x, "ep", [(i, i ^ 1) for i in range(n_ep)])

    wide = moe_tokens.astype(f32)
    local_sq = jnp.sum(wide * wide, axis=1)
    total_sq = sum_ctx(local_sq)
    scale_rows = lax.rsqrt(total_sq / (width * lax.axis_size("ctx")) + norm_eps)
    normed = (wide * scale_rows[:, None] * norm_gain[None, :]).astype(bf16)

    slots = jnp.arange(rows, dtype=jnp.int32)
    pos_right = position(expert_ids, True)
    pos_left = position(expert_ids, False)
    perm_right = (pos_right[None, :] == slots[:, None]).astype(bf16)
    perm_left = (pos_left[None, :] == slots[:, None]).astype(bf16)

    gates = [w_gate[0], partner(w_gate[0])]
    ups = [w_up[0], partner(w_up[0])]
    downs = [w_down[0], partner(w_down[0])]

    held = {}
    for to_right, perm in ((True, perm_right), (False, perm_left)):
        for b, lo, hi in bands:
            block = mm(perm[lo:hi], normed).astype(bf16)
            for k in range(1, nz):
                if to_right:
                    pairs = [(a, a + 1) for a in range(k - 1, nz - 1 - b)]
                else:
                    pairs = [(nz - 1 - a, nz - 2 - a) for a in range(k - 1, nz - 1 - b)]
                if not pairs:
                    break
                block = hop(block, pairs)
                held[to_right, k, b] = block

    def chunk_of(zz, j):
        m = min(zz, nz - 1 - zz)
        if j <= 2 * m:
            return (j % 2 == 1, (j + 1) // 2)
        return (zz > nz - 1 - zz, j - m)

    expert = z

    def picks(ids, scales):
        hits = jnp.any(ids == expert, axis=1)
        at = jnp.arange(rows, dtype=jnp.int32)
        before = hits[None, :] & (at[None, :] < at[:, None])
        slot = jnp.sum(before.astype(jnp.int32), axis=1)
        sel = hits[None, :] & (slot[None, :] == jnp.arange(cap, dtype=jnp.int32)[:, None])
        own = jnp.sum(jnp.where(ids == expert, scales, 0.0), axis=1)
        return sel.astype(bf16), own

    def hidden_of(rows_in, sel):
        parts = jnp.concatenate(
            [mm(rows_in, w) for w in (gates[0], gates[1], ups[0], ups[1])], axis=1
        )
        units = parts.shape[1] // 2

        def act(both):
            return (jax.nn.silu(both[:, :units]) * both[:, units:]).astype(bf16)

        if lax.axis_size("ctx") != 2:
            both = lax.psum_scatter(parts.astype(bf16), "ctx", scatter_dimension=0, tiled=True)
            hid = lax.all_gather(act(both.astype(f32)), "ctx", axis=0, tiled=True)
            return mm_t(sel, hid).astype(bf16)
        theirs = lax.dynamic_slice_in_dim(parts, (1 - ctx) * half, half, 0).astype(bf16)
        mine = lax.dynamic_slice_in_dim(parts, ctx * half, half, 0)
        hid = act(mine + swap_ctx(theirs).astype(f32))
        hid_other = swap_ctx(hid)
        sel_mine = lax.dynamic_slice_in_dim(sel, ctx * half, half, 0)
        sel_other = lax.dynamic_slice_in_dim(sel, (1 - ctx) * half, half, 0)
        return (mm_t(sel_mine, hid) + mm_t(sel_other, hid_other)).astype(bf16)

    fh = w_gate.shape[2]
    step = width // pieces

    def contribution(hid, scale, piece):
        cols = slice(piece * step, (piece + 1) * step)
        out = mm(hid[:, :fh], downs[0][:, cols]) + mm(hid[:, fh:], downs[1][:, cols])
        return out * scale[:, None]

    sel_own, scale_own = picks(expert_ids, route_scale)
    hid_own = hidden_of(mm(sel_own, normed).astype(bf16), sel_own)

    hids = {}
    for j in range(1, nz):
        kinds = [chunk_of(zz, j) for zz in range(nz)]
        distinct = sorted(set(kinds))

        def choose(get):
            value = None
            for kind in distinct:
                here = False
                for zz in range(nz):
                    if kinds[zz] == kind:
                        here = here | (z == zz)
                got = get(kind)
                if got is None:
                    continue
                value = got if value is None else jnp.where(here, got, value)
            return value

        def source_info(kind):
            to_right, k = kind
            return infos[k] if to_right else infos[nz - k]

        chosen = choose(source_info)
        from_left = choose(lambda kind: jnp.full((1,), kind[0], jnp.bool_))[0]
        ids = chosen[:, :top_count].astype(jnp.int32)
        sel, scale = picks(ids, chosen[:, top_count:])
        pos = position(ids, from_left)
        place = (pos[:, None] == slots[None, :]).astype(bf16)
        sel_at = mm(sel, place).astype(bf16)
        scale_at = jnp.sum(jnp.where(pos[:, None] == slots[None, :], scale[:, None], 0.0), axis=0)
        rows_in = None
        for b, lo, hi in bands:
            block = choose(lambda kind: held.get((kind[0], kind[1], b)))
            if block is None:
                continue
            part = mm(sel_at[:, lo:hi], block)
            rows_in = part if rows_in is None else rows_in + part
        hids[j] = (hidden_of(rows_in.astype(bf16), sel_at), scale_at, kinds)

    def chunk_for(to_right, k):
        hid = scale = None
        for j in range(1, nz):
            zs = [zz for zz in range(nz) if hids[j][2][zz] == (to_right, k)]
            if not zs:
                continue
            here = False
            for zz in zs:
                here = here | (z == zz)
            if hid is None:
                hid = jnp.where(here, hids[j][0], 0)
                scale = jnp.where(here, hids[j][1], 0)
            else:
                hid = jnp.where(here, hids[j][0], hid)
                scale = jnp.where(here, hids[j][1], scale)
        return hid, scale

    returned = {}
    for k in range(nz - 1, 0, -1):
        for to_right in (True, False):
            hid, scale = chunk_for(to_right, k)
            for piece in range(pieces):
                acc = contribution(hid, scale, piece)
                for b, lo, hi in bands:
                    value = acc[lo:hi]
                    before = returned.get((to_right, piece, b))
                    if before is not None:
                        value = value + before.astype(f32)
                    pairs = [(a + 1, a) for a in range(k - 1, nz - 1 - b)]
                    if not to_right:
                        pairs = [(nz - 1 - p, nz - 1 - q) for p, q in pairs]
                    if pairs:
                        returned[to_right, piece, b] = hop(value.astype(bf16), pairs)

    outs = []
    for piece in range(pieces):
        acc = contribution(hid_own, scale_own, piece)
        for to_right, perm in ((True, perm_right), (False, perm_left)):
            for b, lo, hi in bands:
                got = returned.get((to_right, piece, b))
                if got is not None:
                    acc = acc + mm_t(perm[lo:hi], got)
        outs.append(acc.astype(bf16))
    moe_out = jnp.concatenate(outs, axis=1)
    attn_out = attention(q_latent, q_rope, latent_keys, rope_keys, w_uv)
    return (attn_out, moe_out)


def expert_kernel(
    nz,
    chunks,
    total_width,
    ql_hbm,
    qr_hbm,
    lk_hbm,
    rk_hbm,
    uv_hbm,
    x_hbm,
    wg_hbm,
    wu_hbm,
    wd_hbm,
    gain_hbm,
    ids_hbm,
    scale_hbm,
    attn_hbm,
    own_hbm,
    right_hbm,
    left_hbm,
    gain_ref,
    ids_ref,
    scale_ref,
    ql,
    qr,
    keys,
    ropes,
    uv,
    attn,
    xs,
    wgu,
    wd,
    ret,
    con,
    theirs,
    mine,
    outgoing,
    scaled,
    squares,
    squares_in,
    routes,
    a_local,
    a_send,
    a_recv,
    local_sem,
    w_send,
    w_recv,
    x_send,
    x_recv,
    r_send,
    r_recv,
    p_send,
    p_recv,
    q_send,
    q_recv,
    t_send,
    t_recv,
    o_sem,
    s_sem,
):
    ep = lax.axis_index("ep")
    z = ep // 2
    core = ep % 2
    ctx = lax.axis_index("ctx")
    rows, width = xs.shape[1], xs.shape[2]
    fh = wgu.shape[2]
    groups = rows // 8
    last = nz - 1
    spans = last * chunks
    half = chunks // 2
    left, right = {"ep": ep - 2}, {"ep": ep + 2}
    across = {"ctx": 1 - ctx}
    beside = {"ep": 2 * z + 1 - core}

    def remote(src, dst, send, recv, device):
        return pltpu.make_async_remote_copy(
            src_ref=src,
            dst_ref=dst,
            send_sem=send,
            recv_sem=recv,
            device_id=device,
            device_id_type=pl.DeviceIdType.MESH,
        )

    barrier = pltpu.get_barrier_semaphore()
    for near, device in ((z > 0, left), (z < last, right)):

        @pl.when(near)
        def _():
            pl.semaphore_signal(
                barrier, inc=1, device_id=device, device_id_type=pl.DeviceIdType.MESH
            )

    for device in (across, beside):
        pl.semaphore_signal(
            barrier, inc=1, device_id=device, device_id_type=pl.DeviceIdType.MESH
        )

    def own_weights(k):
        if k == 0:
            return pltpu.make_async_copy(wg_hbm.at[0], wgu.at[0], local_sem.at[0])
        if k == 1:
            return pltpu.make_async_copy(wu_hbm.at[0], wgu.at[2], local_sem.at[1])
        return pltpu.make_async_copy(wd_hbm.at[0], wd.at[pl.ds(0, fh), :], local_sem.at[2])

    def give_weights(k):
        src = (wg_hbm, wu_hbm, wd_hbm)[k].at[0]
        dst = (wgu.at[1], wgu.at[3], wd.at[pl.ds(fh, fh), :])[k]
        return remote(src, dst, w_send.at[k], w_recv.at[k], beside)

    def own_rows(i):
        return pltpu.make_async_copy(
            x_hbm.at[pl.ds(i * rows, rows), :], xs.at[z * chunks + i], local_sem.at[3 + i]
        )

    def give_rows(i, to_right):
        side = right if to_right else left
        sem = z * chunks + i if to_right else nz * chunks + i
        return remote(
            xs.at[z * chunks + i],
            xs.at[z * chunks + i],
            x_send.at[sem],
            x_recv.at[z * chunks + i],
            side,
        )

    def pass_rows(at, to_right):
        side = right if to_right else left
        return remote(xs.at[at], xs.at[at], x_send.at[at], x_recv.at[at], side)

    def pass_routes(source, to_right):
        side = right if to_right else left
        return remote(
            routes.at[source],
            routes.at[source],
            t_send.at[source if to_right else source + 1],
            t_recv.at[source],
            side,
        )

    seq = ql.shape[0]
    latent = keys.shape[0]
    turn = qr_hbm.shape[1] // uv.shape[0]
    mine_at = pl.ds(pl.multiple_of(ctx * seq, seq), seq)
    key_parts = (
        (lk_hbm, keys.at[:, mine_at]),
        (rk_hbm, ropes.at[0, pl.ds(0, turn), mine_at]),
        (rk_hbm, ropes.at[1, pl.ds(turn, turn), mine_at]),
    )

    def local_attention():
        pairs = key_parts + ((ql_hbm, ql), (qr_hbm, qr), (uv_hbm, uv))
        return [
            pltpu.make_async_copy(src, dst, a_local.at[n]) for n, (src, dst) in enumerate(pairs)
        ]

    def give_keys():
        return [
            remote(src, dst, a_send.at[n], a_recv.at[n], across)
            for n, (src, dst) in enumerate(key_parts)
        ]

    def put_attention():
        return pltpu.make_async_copy(attn, attn_hbm, a_local.at[6])

    def attend(head):
        span = keys.shape[1]
        value = uv.shape[2]
        pair = head // 2
        query = ctx * seq + lax.broadcasted_iota(jnp.int32, (seq, span), 0)
        visible = lax.broadcasted_iota(jnp.int32, (seq, span), 1) <= query
        query_lat = ql[:, pl.ds(pl.multiple_of(head * latent, latent), latent)]
        query_rot = qr[:, pl.ds(pl.multiple_of(pair * 2 * turn, 2 * turn), 2 * turn)]
        rotary = ropes[lax.rem(head, 2)]
        scores = (mm(query_lat, keys[...]) + mm(query_rot, rotary)) * score_scale
        masked = jnp.where(visible, scores, neg_large)
        top = jnp.max(masked, axis=1, keepdims=True)
        weights = jnp.where(visible, jnp.exp(masked - top), 0.0)
        whole = jnp.sum(weights, axis=1, keepdims=True)
        update = lax.dot_general(
            weights.astype(bf16), keys[...], (((1,), (1,)), ((), ())), preferred_element_type=f32
        )
        attn[:, pl.ds(pl.multiple_of(head * value, value), value)] = mm(
            (update / whole).astype(bf16), uv[head]
        ).astype(bf16)

    small = [
        pltpu.make_async_copy(src, dst, s_sem.at[n])
        for n, (src, dst) in enumerate(
            ((ids_hbm, ids_ref), (scale_hbm, scale_ref), (gain_hbm, gain_ref))
        )
    ]
    for copy in small:
        copy.start()
    for i in range(chunks):
        own_rows(i).start()

    @pl.when((z == 0) | (z == last))
    def _():
        pl.semaphore_wait(barrier, 3)

    @pl.when((z > 0) & (z < last))
    def _():
        pl.semaphore_wait(barrier, 4)

    for i in range(half):
        own_rows(i).wait()

        @pl.when(z < last)
        def _():
            give_rows(i, True).start()

        @pl.when(z > 0)
        def _():
            give_rows(i, False).start()

    def give_rest(to_right):
        for i in range(half, chunks):
            give_rows(i, to_right).start()

    ropes[0, turn:, :] = jnp.zeros((turn, ropes.shape[2]), bf16)
    ropes[1, :turn, :] = jnp.zeros((turn, ropes.shape[2]), bf16)
    for copy in small:
        copy.wait()
    for expert in range(nz):
        line = jnp.zeros((1, routes.shape[3]), f32)
        for k in range(ids_ref.shape[0]):
            line = line + jnp.where(
                ids_ref[k : k + 1, :] == expert, scale_ref[k : k + 1, :], 0.0
            )
        routes[z, expert] = line

    @pl.when(z < last)
    def _():
        pass_routes(z, True).start()

    @pl.when(z > 0)
    def _():
        pass_routes(z, False).start()

    for k in range(2):
        own_weights(k).start()
    for i in range(half, chunks):
        own_rows(i).wait()

    @pl.when(z == 0)
    def _():
        give_rest(True)

    @pl.when(z == last)
    def _():
        give_rest(False)

    for copy in local_attention() + give_keys():
        copy.start()
    for k in range(2):
        give_weights(k).start()
    own_weights(2).start()
    give_weights(2).start()
    row_group = lax.broadcasted_iota(jnp.int32, (rows, 128), 0) // 8
    lane = lax.broadcasted_iota(jnp.int32, (rows, 128), 1)
    block = fh if width % fh == 0 else 128

    def spread(packed):
        tall = jnp.broadcast_to(packed[None], (groups, 8, 128)).reshape(rows, 128)
        return jnp.sum(jnp.where(lane == row_group, tall, 0.0), axis=1, keepdims=True)

    def weights_of(source, i):
        tokens = routes.shape[3]
        shape = (rows, tokens)
        wanted = lax.broadcasted_iota(jnp.int32, shape, 0) + i * rows
        hit = lax.broadcasted_iota(jnp.int32, shape, 1) == wanted
        line = jnp.broadcast_to(routes[source, z], shape)
        return jnp.sum(jnp.where(hit, line, 0.0), axis=1, keepdims=True)

    def exchange(at, slot, lane_at):
        return (
            remote(
                outgoing.at[slot, lane_at], theirs.at[at], p_send.at[at], p_recv.at[at], across
            ),
            remote(
                squares.at[slot, lane_at], squares_in.at[at], q_send.at[at], q_recv.at[at], across
            ),
        )

    def normalise(at, slot, lane_at):
        lines = pl.ds(lane_at * rows, rows)

        def columns(n, total):
            cols = pl.ds(pl.multiple_of(n * block, block), block)
            wide = xs[at, :, cols].astype(f32)
            scaled[lines, cols] = (wide * gain_ref[cols][None, :]).astype(bf16)
            square = wide * wide
            for m in range(block // 128):
                total = total + square[:, m * 128 : (m + 1) * 128]
            return total

        total = lax.fori_loop(0, width // block, columns, jnp.zeros((rows, 128), f32))
        column = jnp.sum(total, axis=1, keepdims=True)
        packed = jnp.where(lane == row_group, jnp.broadcast_to(column, (rows, 128)), 0.0)
        squares[slot, lane_at] = jnp.sum(packed.reshape(groups, 8, 128), axis=0)

    def project(t):
        slot = lax.rem(t, LAG + 1)
        places = [place(t, n) for n in range(2)]
        for n, (source, i, there) in enumerate(places):

            @pl.when(there)
            def _():
                normalise(source * chunks + i, slot, n)

        @pl.when(places[0][2] | places[1][2])
        def _():
            @pl.loop(0, 4)
            def _(k):
                part = jnp.dot(scaled[...], wgu[k], preferred_element_type=f32)
                mine[slot, k] = part
                for n in range(2):
                    outgoing[slot, n, k] = part[n * rows : (n + 1) * rows].astype(bf16)

        for n, (source, i, there) in enumerate(places):

            @pl.when(there)
            def _():
                for copy in exchange(source * chunks + i, slot, n):
                    copy.start()

    def activate(source, i, slot, lane_at):
        at = source * chunks + i
        lines = pl.ds(lane_at * rows, rows)
        for copy in exchange(at, slot, lane_at):
            copy.wait()
        square = spread(squares[slot, lane_at] + squares_in[at])
        scale = lax.rsqrt(square / total_width + norm_eps)
        weight = weights_of(source, i)

        @pl.loop(0, 2)
        def _(b):
            gate = (mine[slot, b, lines] + theirs[at, b].astype(f32)) * scale
            up = (mine[slot, b + 2, lines] + theirs[at, b + 2].astype(f32)) * scale
            hid = jax.nn.silu(gate) * up * weight
            scaled[lines, pl.ds(pl.multiple_of(b * fh, fh), fh)] = hid.astype(bf16)

    def expand(t):
        slot = lax.rem(t + LAG + 1, LAG + 1)
        places = [place(t, n) for n in range(2)]
        for n, (source, i, there) in enumerate(places):

            @pl.when(there)
            def _():
                activate(source, i, slot, n)

        @pl.when(places[0][2] | places[1][2])
        def _():
            @pl.loop(0, width // block)
            def _(b):
                cols = pl.ds(pl.multiple_of(b * block, block), block)
                part = jnp.dot(scaled[:, : 2 * fh], wd[:, cols], preferred_element_type=f32)
                for n, (source, i, there) in enumerate(places):

                    @pl.when(there)
                    def _():
                        con[source * chunks + i, :, cols] = part[
                            n * rows : (n + 1) * rows
                        ].astype(bf16)

    def arrival(k, from_left):
        near = z if from_left else last - z
        part = k // half
        late = part >= near
        source = jnp.where(late, part - near, near - 1 - part)
        i = lax.rem(k, half) + jnp.where(late, half, 0)
        there = (k >= 0) & (k < near * chunks)
        return source if from_left else last - source, i, there

    def place(t, lane_at):
        source, i, there = arrival(t, lane_at == 0)
        own_i = t - (spans - chunks)
        own = (own_i >= 0) & (own_i < chunks)
        own = own & ((z < last) if lane_at == 0 else (z == last))
        own = own & jnp.logical_not(there)
        return jnp.where(own, z, source), jnp.where(own, own_i, i), there | own

    def give_back(source, i, to_left, home=False):
        at = source * chunks + i
        to = at if to_left else at + chunks
        side = left if to_left else right
        dst = (right_hbm if to_left else left_hbm) if home else ret.at[to]
        return remote(con.at[at], dst, r_send.at[at], r_recv.at[to], side)

    def send_back(source, i, to_left):
        is_home = (source == (z - 1 if to_left else z + 1)) & (i == chunks - 1)

        @pl.when(is_home)
        def _():
            give_back(source, i, to_left, True).start()

        @pl.when(jnp.logical_not(is_home))
        def _():
            give_back(source, i, to_left).start()

    def put_own(i):
        lines = pl.ds(pl.multiple_of(i * rows, rows), rows)
        return pltpu.make_async_copy(con.at[z * chunks + i], own_hbm.at[lines], o_sem.at[i])

    def await_back(source, i, to_left):
        at = source * chunks + i
        to = at if to_left else at + chunks
        remote(con.at[at], ret.at[to], r_send.at[at], r_recv.at[to], left).wait_recv()
        return to

    def add_back(source, i, tos):
        at = source * chunks + i

        @pl.loop(0, width // block)
        def _(n):
            cols = pl.ds(pl.multiple_of(n * block, block), block)
            value = con[at, :, cols].astype(f32)
            for to in tos:
                value = value + ret[to, :, cols].astype(f32)
            con[at, :, cols] = value.astype(bf16)

    def slot_step(t, carry):
        for to_right in (True, False):
            source, i, there = arrival(t, to_right)
            onward = (z < last) if to_right else (z > 0)
            near = z if to_right else last - z

            @pl.when(there)
            def _():
                at = source * chunks + i
                pass_rows(at, to_right).wait_recv()

                @pl.when(onward)
                def _():
                    pass_rows(at, to_right).start()

                @pl.when(i == half - 1)
                def _():
                    pass_routes(source, to_right).wait_recv()

                    @pl.when(onward)
                    def _():
                        pass_routes(source, to_right).start()

            @pl.when(onward & (near > 0) & (t == near * chunks - 1))
            def _():
                give_rest(to_right)

        @pl.when(t == 0)
        def _():
            for k in range(2):
                own_weights(k).wait()
                give_weights(k).wait()

        project(t)

        @pl.when(t == LAG)
        def _():
            own_weights(2).wait()
            give_weights(2).wait()

        heads = uv.shape[0]

        @pl.when(t == chunks)
        def _():
            for copy in local_attention():
                copy.wait()
            for copy in give_keys():
                copy.wait()

        @pl.when((t >= chunks) & (t < chunks + heads))
        def _():
            attend(t - chunks)

        @pl.when(t == chunks + heads)
        def _():
            put_attention().start()

        expand(t - LAG)

        @pl.when(t - LAG == spans - 1)
        def _():
            put_own(chunks - 1).start()

        for to_left in (True, False):
            near = z if to_left else last - z
            source, i, there = arrival(t - LAG, to_left)

            @pl.when(there & (near == last))
            def _():
                send_back(source, i, to_left)

            k = t + half - (nz - near) * chunks
            source_back, i_back, there_back = arrival(k, to_left)

            @pl.when(there_back & (near < last))
            def _():
                to = await_back(source_back, i_back, to_left)
                add_back(source_back, i_back, [to])
                send_back(source_back, i_back, to_left)

        return carry

    lax.fori_loop(0, nz * chunks, slot_step, 0)

    for where, sides in (
        (z == 0, (True,)),
        (z == last, (False,)),
        ((z > 0) & (z < last), (True, False)),
    ):

        @pl.when(where)
        def _():
            @pl.loop(0, chunks - 1)
            def _(i):
                add_back(z, i, [await_back(z, i, to_left) for to_left in sides])
                put_own(i).start()

    put_attention().wait()
    for i in range(chunks):

        @pl.when(z < last)
        def _():
            give_rows(i, True).wait_send()

        @pl.when(z > 0)
        def _():
            give_rows(i, False).wait_send()

    @pl.when(z < last)
    def _():
        pass_routes(z, True).wait_send()

    @pl.when(z > 0)
    def _():
        pass_routes(z, False).wait_send()

    def settle(t, carry):
        for to_right in (True, False):
            source, i, there = arrival(t, to_right)
            onward = (z < last) if to_right else (z > 0)

            @pl.when(there)
            def _():
                give_back(source, i, to_right).wait_send()

                @pl.when(onward)
                def _():
                    pass_rows(source * chunks + i, to_right).wait_send()

                @pl.when(onward & (i == half - 1))
                def _():
                    pass_routes(source, to_right).wait_send()

        return carry

    lax.fori_loop(0, spans, settle, 0)

    for i in range(chunks):
        put_own(i).wait()

    @pl.when(z < last)
    def _():
        give_back(z, chunks - 1, True, True).wait_recv()

    @pl.when(z > 0)
    def _():
        give_back(z, chunks - 1, False, True).wait_recv()


def gather_kernel(
    last,
    chunks,
    attn_in,
    own_in,
    right_in,
    left_in,
    attn_out,
    out_hbm,
    attn,
    own,
    right,
    left,
    sem_in,
    sem_out,
):
    z = lax.axis_index("ep") // 2
    rows, width = right.shape

    def take(i):
        return pltpu.make_async_copy(own_in.at[pl.ds(i * rows, rows)], own.at[i], sem_in.at[i])

    def put(i):
        return pltpu.make_async_copy(own.at[i], out_hbm.at[pl.ds(i * rows, rows)], sem_out.at[i])

    final = chunks - 1
    take_right = pltpu.make_async_copy(right_in, right, sem_in.at[chunks])
    take_left = pltpu.make_async_copy(left_in, left, sem_in.at[chunks + 1])
    take_attn = pltpu.make_async_copy(attn_in, attn, sem_in.at[chunks + 2])
    put_attn = pltpu.make_async_copy(attn, attn_out, sem_out.at[chunks])
    take(final).start()
    take_right.start()
    take_left.start()
    take_attn.start()
    for i in range(final):
        take(i).start()
    take(final).wait()
    take_right.wait()
    take_left.wait()
    block = 512 if width % 512 == 0 else 128

    @pl.loop(0, width // block)
    def _(n):
        cols = pl.ds(pl.multiple_of(n * block, block), block)
        value = own[final, :, cols].astype(f32)
        value = value + jnp.where(z < last, right[:, cols].astype(f32), 0.0)
        value = value + jnp.where(z > 0, left[:, cols].astype(f32), 0.0)
        own[final, :, cols] = value.astype(bf16)

    put(final).start()
    take_attn.wait()
    put_attn.start()
    for i in range(final):
        take(i).wait()
        put(i).start()
    put_attn.wait()
    for i in range(chunks):
        put(i).wait()


def expert_scratch(nz, rows, width, fh, seq, heads, latent, turn, value, tokens, top):
    jobs = nz * CHUNKS
    dma = pltpu.SemaphoreType.DMA
    return [
        pltpu.VMEM((width,), f32),
        pltpu.VMEM((top, tokens), jnp.int32),
        pltpu.VMEM((top, tokens), f32),
        pltpu.VMEM((seq, heads * latent), bf16),
        pltpu.VMEM((seq, heads * turn), bf16),
        pltpu.VMEM((latent, 2 * seq), bf16),
        pltpu.VMEM((2, 2 * turn, 2 * seq), bf16),
        pltpu.VMEM((heads, latent, value), bf16),
        pltpu.VMEM((seq, heads * value), bf16),
        pltpu.VMEM((jobs, rows, width), bf16),
        pltpu.VMEM((4, width, fh), bf16),
        pltpu.VMEM((2 * fh, width), bf16),
        pltpu.VMEM((jobs + CHUNKS, rows, width), bf16),
        pltpu.VMEM((jobs, rows, width), bf16),
        pltpu.VMEM((jobs, 4, rows, fh), bf16),
        pltpu.VMEM((LAG + 1, 4, 2 * rows, fh), f32),
        pltpu.VMEM((LAG + 1, 2, 4, rows, fh), bf16),
        pltpu.VMEM((2 * rows, width), bf16),
        pltpu.VMEM((LAG + 1, 2, 8, 128), f32),
        pltpu.VMEM((jobs, 8, 128), f32),
        pltpu.VMEM((nz, nz, 1, tokens), f32),
        dma((7,)),
        dma((3,)),
        dma((3,)),
        dma((3 + CHUNKS,)),
        dma((3,)),
        dma((3,)),
        dma((jobs + CHUNKS,)),
        dma((jobs,)),
        dma((jobs,)),
        dma((jobs + CHUNKS,)),
        dma((jobs,)),
        dma((jobs,)),
        dma((jobs,)),
        dma((jobs,)),
        dma((nz + 1,)),
        dma((nz,)),
        dma((CHUNKS,)),
        dma((3,)),
    ]


def scratch_bytes(shapes):
    total = 0
    for s in shapes:
        if s.memory_space == pltpu.VMEM:
            n = jnp.dtype(s.dtype).itemsize
            for d in s.shape:
                n *= d
            total += n
    return total


def sizes(latent_keys, rope_keys, w_uv, moe_tokens, expert_ids, w_gate):
    heads, latent, value = w_uv.shape
    tokens, width = moe_tokens.shape
    return dict(
        nz=lax.axis_size("ep") // 2,
        rows=tokens // CHUNKS,
        width=width,
        fh=w_gate.shape[2],
        seq=latent_keys.shape[1],
        heads=heads,
        latent=latent,
        turn=rope_keys.shape[0],
        value=value,
        tokens=tokens,
        top=expert_ids.shape[1],
    )


def fits(n, w_gate):
    n_ep = lax.axis_size("ep")
    if lax.axis_size("ctx") != 2 or n_ep % 2 or n["nz"] < 2 or w_gate.shape[0] != 1:
        return False
    if n["tokens"] % (16 * CHUNKS) or n["rows"] > 1024 or n["heads"] > (n["nz"] - 1) * CHUNKS:
        return False
    lanes = ("width", "fh", "seq", "latent", "value", "tokens")
    if any(n[name] % 128 for name in lanes) or n["turn"] != 64 or n["heads"] % 2:
        return False
    return scratch_bytes(expert_scratch(**n)) < VMEM_BYTES - 2**20


def fused(n, attention_in, moe_in):
    moe_tokens, norm_gain, expert_ids, route_scale, w_gate, w_up, w_down = moe_in
    anywhere = pl.BlockSpec(memory_space=pl.ANY)
    total = n["width"] * lax.axis_size("ctx")
    attn_shape = jax.ShapeDtypeStruct((n["seq"], n["heads"] * n["value"]), bf16)
    rows_shape = jax.ShapeDtypeStruct((n["tokens"], n["width"]), bf16)
    last_shape = jax.ShapeDtypeStruct((n["rows"], n["width"]), bf16)
    parts = pl.pallas_call(
        functools.partial(expert_kernel, n["nz"], CHUNKS, total),
        out_shape=(attn_shape, rows_shape, last_shape, last_shape),
        in_specs=[anywhere] * 12,
        out_specs=(anywhere,) * 4,
        scratch_shapes=expert_scratch(**n),
        compiler_params=pltpu.CompilerParams(
            collective_id=0, has_side_effects=True, vmem_limit_bytes=VMEM_BYTES
        ),
    )(*attention_in, moe_tokens, w_gate, w_up, w_down, norm_gain, expert_ids.T, route_scale.T)
    dma = pltpu.SemaphoreType.DMA
    return pl.pallas_call(
        functools.partial(gather_kernel, n["nz"] - 1, CHUNKS),
        out_shape=(attn_shape, rows_shape),
        in_specs=[anywhere] * 4,
        out_specs=(anywhere, anywhere),
        scratch_shapes=[
            pltpu.VMEM(attn_shape.shape, bf16),
            pltpu.VMEM((CHUNKS, n["rows"], n["width"]), bf16),
            pltpu.VMEM(last_shape.shape, bf16),
            pltpu.VMEM(last_shape.shape, bf16),
            dma((CHUNKS + 3,)),
            dma((CHUNKS + 1,)),
        ],
        compiler_params=pltpu.CompilerParams(vmem_limit_bytes=VMEM_BYTES),
    )(*parts)


def body(
    q_latent,
    q_rope,
    latent_keys,
    rope_keys,
    w_uv,
    moe_tokens,
    norm_gain,
    expert_ids,
    route_scale,
    w_gate,
    w_up,
    w_down,
):
    n = sizes(latent_keys, rope_keys, w_uv, moe_tokens, expert_ids, w_gate)
    if not fits(n, w_gate):
        return hop_body(
            q_latent,
            q_rope,
            latent_keys,
            rope_keys,
            w_uv,
            moe_tokens,
            norm_gain,
            expert_ids,
            route_scale,
            w_gate,
            w_up,
            w_down,
        )
    attention_in = (q_latent, q_rope, latent_keys, rope_keys, w_uv)
    moe_in = (moe_tokens, norm_gain, expert_ids, route_scale, w_gate, w_up, w_down)
    return fused(n, attention_in, moe_in)


def solution(mesh):
    return jax.shard_map(
        body,
        mesh=mesh,
        in_specs=(
            P(("group", "ctx"), "ep"),
            P(("group", "ctx"), "ep"),
            P("group", "ctx"),
            P("group", "ctx"),
            P("ep", None, None),
            P(("group", "ep"), "ctx"),
            P("ctx"),
            P(("group", "ep"), None),
            P(("group", "ep"), None),
            P("ep", "ctx", None),
            P("ep", "ctx", None),
            P("ep", None, "ctx"),
        ),
        out_specs=(P(("group", "ctx"), "ep"), P(("group", "ep"), "ctx")),
        check_vma=False,
    )
```
